16 devices in a mesh: data: 2 (over y, z), seq: 8 (over x, core).
Axes of the slice: x: 4, y: 2, z: 1, core: 2. Of those that a mesh axis runs over, the one named last changes fastest.
The devices are a block of a 4x4x8 slice.
Arguments:
- x_tokens: bfloat16 [128, 512, 768], P('data', 'seq'), parts along dimension 0
- lengths: int32 [128], P('data'), parts along dimension 0
- phi_slots: bfloat16 [768, 128], replicated
- scale_g: float32 [], replicated
- w_in: bfloat16 [128, 768, 3072], P('seq')
- w_out: bfloat16 [128, 3072, 768], P('seq')
- ws_in: bfloat16 [768, 3072], replicated
- ws_out: bfloat16 [3072, 768], replicated
Outputs:
- output: bfloat16 [128, 512, 768], P('data', 'seq'), parts along dimension 0
There are 2 independent parts. The reference program is written for one: setup_inputs(seed, part) draws one part's arguments, and reference() takes and returns one part's arrays. A program takes and returns all parts, laid end to end along the dimension named above; an argument that names none is the same for every part.
All inputs are finite; a program needn't handle non-finite values.
Results may differ from the reference program's by a relative error of at most 0.0133919.
Values are sent between devices in bfloat16 or wider.
A program may use at most 768 MiB of HBM per device.

```python
import jax
import jax.numpy as jnp
from jax import lax

SEQ_BATCH = 64
SEQ_LEN = 512
MODEL_DIM = 768
EXPERT_FF = 3072
NUM_EXPERTS = 128
EXPERT_SLOTS = 1
SHARED_FF = 3072
SLOT_TOTAL = NUM_EXPERTS * EXPERT_SLOTS
NORM_EPS = 1e-6
NEG_BIG = -1e30


def setup_inputs(seed: int = 0, part: int = 0) -> dict:
    root_key = jax.random.key(seed)
    shared_keys = jax.random.split(root_key, 6)
    part_keys = jax.random.split(jax.random.fold_in(root_key, part), 5)
    phi_wide = jax.random.normal(shared_keys[0], (MODEL_DIM, SLOT_TOTAL), jnp.float32)
    phi_unit = phi_wide / jnp.sqrt(jnp.sum(phi_wide * phi_wide, axis=0, keepdims=True))
    slot_pick = jax.random.randint(part_keys[0], (SEQ_BATCH, SEQ_LEN), 0, SLOT_TOTAL)
    align_amp = jax.random.uniform(part_keys[1], (SEQ_BATCH, SEQ_LEN, 1), jnp.float32, 0.0, 2.0)
    noise_part = jax.random.normal(part_keys[2], (SEQ_BATCH, SEQ_LEN, MODEL_DIM), jnp.float32)
    x_wide = noise_part + jnp.take(phi_unit.T, slot_pick, axis=0) * (align_amp * MODEL_DIM ** 0.5)
    base_len = jax.random.randint(part_keys[3], (SEQ_BATCH,), 1, SEQ_LEN + 1)
    full_idx = jax.random.randint(part_keys[4], (), 0, SEQ_BATCH)
    lengths = jnp.where(jnp.arange(SEQ_BATCH) == full_idx, SEQ_LEN, base_len).astype(jnp.int32)
    scale_g = jax.random.uniform(shared_keys[1], (), jnp.float32, 4.0, 8.0)
    w_in = jax.random.normal(shared_keys[2], (NUM_EXPERTS, MODEL_DIM, EXPERT_FF), jnp.float32) * MODEL_DIM ** -0.5
    w_out = jax.random.normal(shared_keys[3], (NUM_EXPERTS, EXPERT_FF, MODEL_DIM), jnp.float32) * (2.0 * EXPERT_FF ** -0.5)
    ws_in = jax.random.normal(shared_keys[4], (MODEL_DIM, SHARED_FF), jnp.float32)
    ws_out = jax.random.normal(shared_keys[5], (SHARED_FF, MODEL_DIM), jnp.float32) * (0.25 * SHARED_FF ** -0.5)
    return {'x_tokens': x_wide.astype(jnp.bfloat16), 'lengths': lengths, 'phi_slots': phi_wide.astype(jnp.bfloat16), 'scale_g': scale_g, 'w_in': w_in.astype(jnp.bfloat16), 'w_out': w_out.astype(jnp.bfloat16), 'ws_in': ws_in.astype(jnp.bfloat16), 'ws_out': ws_out.astype(jnp.bfloat16)}


def unit_rows(values, axis_id):
    wide_vals = values.astype(jnp.float32)
    return wide_vals / jnp.sqrt(jnp.sum(wide_vals * wide_vals, axis=axis_id, keepdims=True) + NORM_EPS)


def reference(x_tokens, lengths, phi_slots, scale_g, w_in, w_out, ws_in, ws_out):
    phi_norm = (scale_g * unit_rows(phi_slots, 0)).astype(jnp.bfloat16)
    positions = jnp.arange(SEQ_LEN)

    def seq_logits(x_seq):
        x_unit = unit_rows(x_seq, 1).astype(jnp.bfloat16)
        return x_unit, jnp.dot(x_unit, phi_norm, preferred_element_type=jnp.float32)

    def dispatch(inputs):
        x_seq, seq_len = inputs
        x_unit, logits = seq_logits(x_seq)
        valid_mask = (positions < seq_len)[:, None]
        col_max = jnp.max(jnp.where(valid_mask, logits, NEG_BIG), axis=0)
        weights = jnp.where(valid_mask, jnp.exp(logits - col_max[None, :]), 0.0)
        col_sum = jnp.sum(weights, axis=0)
        slot_num = jnp.dot(weights.astype(jnp.bfloat16).T, x_seq, preferred_element_type=jnp.float32)
        return (slot_num / col_sum[:, None]).astype(jnp.bfloat16)

    slot_in = lax.map(dispatch, (x_tokens, lengths))
    expert_in = jnp.transpose(slot_in.reshape(SEQ_BATCH, NUM_EXPERTS, EXPERT_SLOTS, MODEL_DIM), (1, 0, 2, 3)).reshape(NUM_EXPERTS, SEQ_BATCH * EXPERT_SLOTS, MODEL_DIM)

    def expert_ffn(inputs):
        expert_rows, w_first, w_second = inputs
        hidden = jax.nn.gelu(jnp.dot(expert_rows, w_first, preferred_element_type=jnp.float32), approximate=True).astype(jnp.bfloat16)
        return jnp.dot(hidden, w_second, preferred_element_type=jnp.float32).astype(jnp.bfloat16)

    expert_out = lax.map(expert_ffn, (expert_in, w_in, w_out))
    slot_out = jnp.transpose(expert_out.reshape(NUM_EXPERTS, SEQ_BATCH, EXPERT_SLOTS, MODEL_DIM), (1, 0, 2, 3)).reshape(SEQ_BATCH, SLOT_TOTAL, MODEL_DIM)

    def combine(inputs):
        x_seq, slot_seq = inputs
        x_unit, logits = seq_logits(x_seq)
        mix_weights = jax.nn.softmax(logits, axis=-1).astype(jnp.bfloat16)
        moe_part = jnp.dot(mix_weights, slot_seq, preferred_element_type=jnp.float32)
        hid_shared = jax.nn.gelu(jnp.dot(x_unit, ws_in, preferred_element_type=jnp.float32), approximate=True).astype(jnp.bfloat16)
        dense_part = jnp.dot(hid_shared, ws_out, preferred_element_type=jnp.float32)
        return (moe_part + dense_part).astype(jnp.bfloat16)

    return lax.map(combine, (x_tokens, slot_out))
```

```python
import functools

import jax
import jax.numpy as jnp
from jax import lax
from jax.experimental import pallas as pl
from jax.experimental.pallas import tpu as pltpu
from jax.sharding import PartitionSpec as P

NORM_EPS = 1e-6
NEG_BIG = -1e30
F32 = jnp.float32
BF16 = jnp.bfloat16
MESH = pl.DeviceIdType.MESH
LANES = 128
NGRP = 2
NCHUNK = 4
ER = 8
VMEM_BYTES = 67043328

D2D, TUP, TDN, RUP, RDN, SUP, SDN = range(7)
OUP, ODN, OPA, FUP, FDN, PUP, PDN, PLO, PHI = range(9)


def unit_rows(values, axis_id):
    wide_vals = values.astype(F32)
    return wide_vals / jnp.sqrt(jnp.sum(wide_vals * wide_vals, axis=axis_id, keepdims=True) + NORM_EPS)


def dot(a, b):
    return jnp.dot(a, b, preferred_element_type=F32)


def gelu(v):
    return jax.nn.gelu(v, approximate=True)


def front_kernel(tok, len_ref, x_ref, phi_ref, xn_ref, lm_ref, mix_ref, pm_ref):
    blk = pl.program_id(0)
    first = lax.axis_index('seq') * tok
    pairs = pm_ref.shape[0]
    rows, cols = 2 * tok, phi_ref.shape[1]

    def body(p, _):
        sl = pl.ds(pl.multiple_of(p * rows, rows), rows)
        x = x_ref[sl, :].astype(F32)
        inv = lax.rsqrt(jnp.sum(x * x, axis=1, keepdims=True) + NORM_EPS)
        xn = (x * inv).astype(BF16)
        xn_ref[sl, :] = xn
        logits = dot(xn, phi_ref[...])
        seq0 = 2 * (blk * pairs + p)
        ri = lax.broadcasted_iota(jnp.int32, (rows, cols), 0)
        ci = lax.broadcasted_iota(jnp.int32, (rows, cols), 1)
        odd = ri >= tok
        same = jnp.where(odd, 1, 0) == ((ci >> 3) & 1)
        lim = jnp.where(odd, len_ref[seq0 + 1], len_ref[seq0])
        valid = (first + (ri & (tok - 1))) < lim
        own = jnp.where(same, logits, NEG_BIG)
        top = jnp.max(own, axis=1, keepdims=True)
        ex = jnp.exp(own - top)
        mix_ref[sl, :] = (ex / jnp.sum(ex, axis=1, keepdims=True)).astype(BF16)
        lm = jnp.where(valid, own, NEG_BIG)
        lm_ref[sl, :] = lm
        pm_ref[pl.ds(p, 1), :] = jnp.max(lm, axis=0, keepdims=True)
        return 0

    lax.fori_loop(0, pairs, body, 0)


def mega_kernel(n, x_hbm, lm_hbm, xn_hbm, pm, wsi_hbm, wso_hbm, w1_hbm, w2_hbm,
                g_hbm, y2_hbm,
                part, dbuf, tbuf, rbuf, wsi, wso, w1b, w2b, xb, lb, xnb, y2b, sbuf, yb,
                mxb, mx, zs, zt, zb, zo,
                rs_s, rs_r, ag_s, ag_r, mx_s, mx_r, z_s, z_r, xl_sem, ws_sem, w_sem, xn_sem, y2_sem, loc_sem):
    me = lax.axis_index('seq')
    chip, core = me // 2, me % 2
    chips = n // 2
    mate = chip * 2 + (1 - core)
    cup, cdn, cop = (chip + 1) % chips, (chip + chips - 1) % chips, (chip + 2) % chips
    up, dn = cup * 2 + core, cdn * 2 + core
    npair = pm.shape[0]
    pc = npair // NCHUNK
    ph = pc // 2
    rows = lb.shape[1] // pc
    dwidth = xb.shape[2]
    ntile = dwidth // LANES
    dtok = xnb.shape[1]
    dtiles = y2_hbm.shape[0] // dtok

    def rdma(src, dst, ss, rs, dev):
        return pltpu.make_async_remote_copy(src_ref=src, dst_ref=dst, send_sem=ss, recv_sem=rs,
                                            device_id={'seq': dev}, device_id_type=MESH)

    def xl_load(c, slot):
        ps = pl.ds(pl.multiple_of(c * pc * rows, pc * rows), pc * rows)
        return (pltpu.make_async_copy(x_hbm.at[ps, :], xb.at[slot], xl_sem.at[0, slot]),
                pltpu.make_async_copy(lm_hbm.at[ps, :], lb.at[slot], xl_sem.at[1, slot]))

    def w_load(e, slot):
        return (pltpu.make_async_copy(w1_hbm.at[e], w1b.at[slot], w_sem.at[0, slot]),
                pltpu.make_async_copy(w2_hbm.at[e], w2b.at[slot], w_sem.at[1, slot]))

    def ws_load():
        return (pltpu.make_async_copy(wsi_hbm, wsi, ws_sem.at[0]),
                pltpu.make_async_copy(wso_hbm, wso, ws_sem.at[1]))

    def xn_load(i, slot):
        ps = pl.ds(pl.multiple_of(i * dtok, dtok), dtok)
        return pltpu.make_async_copy(xn_hbm.at[ps, :], xnb.at[slot], xn_sem.at[slot])

    def y2_store(i, slot):
        ps = pl.ds(pl.multiple_of(i * dtok, dtok), dtok)
        return pltpu.make_async_copy(y2b.at[slot], y2_hbm.at[ps, :], y2_sem.at[slot])

    def start(copies):
        for cp in copies:
            cp.start()

    def all_of(c):
        return pl.ds(c * pc, pc)

    def lo_of(c):
        return pl.ds(c * pc, ph)

    def hi_of(c):
        return pl.ds(c * pc + ph, ph)

    def rs(kind, g, c):
        ss, rr = rs_s.at[kind, g, c], rs_r.at[kind, g, c]
        mine = part.at[g, core]
        if kind == D2D:
            return rdma(part.at[g, 1 - core, :, all_of(c)], dbuf.at[g, :, all_of(c)], ss, rr, mate)
        if kind == TUP:
            return rdma(mine.at[cop, lo_of(c)], tbuf.at[0, g, pl.ds(c * ph, ph)], ss, rr, up)
        if kind == TDN:
            return rdma(mine.at[cop, hi_of(c)], tbuf.at[1, g, pl.ds(c * ph, ph)], ss, rr, dn)
        if kind == RUP:
            return rdma(mine.at[cup, hi_of(c)], rbuf.at[0, g, hi_of(c)], ss, rr, up)
        if kind == RDN:
            return rdma(mine.at[cdn, lo_of(c)], rbuf.at[1, g, lo_of(c)], ss, rr, dn)
        if kind == SUP:
            return rdma(mine.at[cup, lo_of(c)], rbuf.at[0, g, lo_of(c)], ss, rr, up)
        return rdma(mine.at[cdn, hi_of(c)], rbuf.at[1, g, hi_of(c)], ss, rr, dn)

    def stage1(g, c):
        rs(D2D, g, c).wait_recv()

        def body(i, _):
            q = c * pc + i
            a = part[g, core, :, q].astype(F32) + dbuf[g, :, q].astype(F32)
            part[g, core, :, q] = a.astype(BF16)
            return 0

        lax.fori_loop(0, pc, body, 0)
        for kind in (TUP, TDN, RUP, RDN):
            rs(kind, g, c).start()

    def stage2(g, c):
        for kind, nxt, dst, off, d in ((TUP, SUP, cup, 0, 0), (TDN, SDN, cdn, ph, 1)):
            rs(kind, g, c).wait_recv()

            def body(i, _):
                q = c * pc + off + i
                a = part[g, core, dst, q].astype(F32) + tbuf[d, g, c * ph + i].astype(F32)
                part[g, core, dst, q] = a.astype(BF16)
                return 0

            lax.fori_loop(0, ph, body, 0)
            rs(nxt, g, c).start()

    def stage3(g, c):
        for kind in (RUP, RDN, SUP, SDN):
            rs(kind, g, c).wait_recv()
        zg = zo[...]
        lane = lax.broadcasted_iota(jnp.int32, zg.shape, 1)

        def body(i, _):
            q = c * pc + i
            z = jnp.sum(jnp.where(lane == g * npair + q, zg, 0.0), axis=1, keepdims=True)
            a = part[g, core, chip, q].astype(F32) + rbuf[0, g, q].astype(F32) + rbuf[1, g, q].astype(F32)
            a = a / z
            for j in range(ntile):
                sbuf[j, pl.ds(pl.multiple_of(q * 16, 16), 16), :] = a[:, j * LANES:(j + 1) * LANES]
            return 0

        lax.fori_loop(0, pc, body, 0)

    def ag(kind, g, c):
        ss, rr = ag_s.at[kind, g, c], ag_r.at[kind, g, c]
        if kind in (OUP, ODN, OPA):
            return rdma(yb.at[g, all_of(c)], g_hbm.at[g, core, chip, all_of(c)], ss, rr,
                        {OUP: up, ODN: dn, OPA: mate}[kind])
        origin, part_of, dev = {FUP: (cdn, lo_of, up), FDN: (cup, hi_of, dn),
                                PUP: (cdn, all_of, mate), PDN: (cup, all_of, mate),
                                PLO: (cop, lo_of, mate), PHI: (cop, hi_of, mate)}[kind]
        ref = g_hbm.at[g, core, origin, part_of(c)]
        return rdma(ref, ref, ss, rr, dev)

    def own_copy(g, c):
        return pltpu.make_async_copy(yb.at[g, all_of(c)], g_hbm.at[g, core, chip, all_of(c)], loc_sem.at[g, c])

    def send_own(g):
        def body(q, _):
            for j in range(ntile):
                yb[g, q, :, j * LANES:(j + 1) * LANES] = sbuf[j, pl.ds(pl.multiple_of(q * 16, 16), 16), :].astype(BF16)
            return 0

        for c in range(NCHUNK):
            lax.fori_loop(c * pc, (c + 1) * pc, body, 0)
            for kind in (OUP, ODN, OPA):
                ag(kind, g, c).start()
            own_copy(g, c).start()

    def relay1(g, c):
        ag(OUP, g, c).wait_recv()
        ag(FUP, g, c).start()
        ag(PUP, g, c).start()
        ag(ODN, g, c).wait_recv()
        ag(FDN, g, c).start()
        ag(PDN, g, c).start()

    def relay2(g, c):
        ag(FUP, g, c).wait_recv()
        ag(PLO, g, c).start()
        ag(FDN, g, c).wait_recv()
        ag(PHI, g, c).start()

    def dense_tile(i):
        slot = i % 2
        xn_load(i, slot).wait()
        xt = xnb[slot]
        hidden = wsi.shape[1]
        step = min(hidden, 768)
        acc = None
        for f in range(0, hidden, step):
            h = gelu(dot(xt, wsi[:, f:f + step])).astype(BF16)
            o = dot(h, wso[f:f + step, :])
            acc = o if acc is None else acc + o

        @pl.when(i >= 2)
        def _():
            y2_store(i - 2, slot).wait()

        y2b[slot] = acc
        y2_store(i, slot).start()

        @pl.when(i + 2 < dtiles)
        def _():
            xn_load(i + 2, slot).start()

    def expert(g, e, total):
        idx = g * ER + e
        slot = idx % 2
        xin = jnp.concatenate([sbuf[j, pl.ds(e, 2 * npair, stride=ER), :] for j in range(ntile)], axis=1).astype(BF16)
        l1, l2 = w_load(idx, slot)
        l1.wait()
        l2.wait()
        hidden = w1b.shape[2]
        step = min(hidden, 768)
        acc = None
        for f in range(0, hidden, step):
            h = gelu(dot(xin, w1b[slot, :, f:f + step])).astype(BF16)
            o = dot(h, w2b[slot, f:f + step, :])
            acc = o if acc is None else acc + o
        for j in range(ntile):
            sbuf[j, pl.ds(e, 2 * npair, stride=ER), :] = acc[:, j * LANES:(j + 1) * LANES]

        @pl.when(idx + 2 < total)
        def _():
            start(w_load(idx + 2, slot))

    start(xl_load(0, 0))
    start(xl_load(1, 1))
    barrier = pltpu.get_barrier_semaphore()
    for k in range(1, n):
        pl.semaphore_signal(barrier, inc=1, device_id={'seq': lax.rem(me + k, n)}, device_id_type=MESH)
    zs[...] = jnp.zeros_like(zs)
    pl.semaphore_wait(barrier, n - 1)

    def mx_msg(k):
        return rdma(pm, mxb.at[me], mx_s.at[k - 1], mx_r.at[k - 1], lax.rem(me + k, n))

    for k in range(1, n):
        mx_msg(k).start()
    start(ws_load())
    xn_load(0, 0).start()
    xn_load(1, 1).start()
    for k in range(1, n):
        mx_msg(k).wait_recv()
    top = pm[...]
    for k in range(1, n):
        top = jnp.maximum(top, mxb[lax.rem(me + n - k, n)])
    mx[...] = top

    half = lb.shape[2] // 2

    def num_chunk(c, _):
        slot = c % 2
        for cp in xl_load(c, slot):
            cp.wait()

        def body(i, _):
            q = c * pc + i
            sl = pl.ds(pl.multiple_of(i * rows, rows), rows)
            e = jnp.exp(lb[slot, sl, :] - mx[pl.ds(q, 1), :])
            z = jnp.sum(e, axis=0, keepdims=True)
            zs[pl.ds(q, 1), :] = z[:, :half]
            zs[pl.ds(npair + q, 1), :] = z[:, half:]
            num = lax.dot_general(e.astype(BF16), xb[slot, sl, :], (((0,), (0,)), ((), ())),
                                  preferred_element_type=F32)
            part[:, :, :, q] = num.astype(BF16).reshape(NGRP, 2, chips, 16, dwidth)
            return 0

        lax.fori_loop(0, pc, body, 0)
        for g in range(NGRP):
            rs(D2D, g, c).start()

        @pl.when(c + 2 < NCHUNK)
        def _():
            start(xl_load(c + 2, slot))

        @pl.when(c >= 1)
        def _():
            stage1(0, c - 1)

        return 0

    lax.fori_loop(0, NCHUNK, num_chunk, 0)
    start(w_load(0, 0))
    start(w_load(1, 1))
    stage1(0, NCHUNK - 1)

    zt[...] = zs[...].T.reshape(zt.shape)

    def z_msg(k):
        dev = lax.rem(me + k, n)
        return rdma(zt.at[dev % 2, dev // 2], zb.at[me], z_s.at[k - 1], z_r.at[k - 1], dev)

    for k in range(1, n):
        z_msg(k).start()
    for cp in ws_load():
        cp.wait()

    def dense_a(i, _):
        dense_tile(i)

        @pl.when(i < NCHUNK)
        def _():
            stage2(0, i)

        @pl.when((i >= NCHUNK) & (i < 2 * NCHUNK))
        def _():
            stage1(1, i - NCHUNK)

        return 0

    lax.fori_loop(0, dtiles // 2, dense_a, 0)

    for k in range(1, n):
        z_msg(k).wait_recv()
    ztot = zt[core, chip]
    for k in range(1, n):
        ztot = ztot + zb[lax.rem(me + n - k, n)]
    zo[...] = ztot

    def run3(g):
        def body(c, _):
            stage3(g, c)
            return 0

        lax.fori_loop(0, NCHUNK, body, 0)

    run3(0)

    total = NGRP * ER

    def experts_a(e, _):
        expert(0, e, total)

        @pl.when(e < NCHUNK)
        def _():
            stage2(1, e)

        return 0

    lax.fori_loop(0, ER, experts_a, 0)
    send_own(0)
    run3(1)

    def experts_b(e, _):
        expert(1, e, total)

        @pl.when(e < NCHUNK)
        def _():
            relay1(0, e)

        @pl.when(e >= NCHUNK)
        def _():
            relay2(0, e - NCHUNK)

        return 0

    lax.fori_loop(0, ER, experts_b, 0)
    send_own(1)

    def dense_b(i, _):
        dense_tile(dtiles // 2 + i)

        @pl.when(i < NCHUNK)
        def _():
            relay1(1, i)

        @pl.when((i >= NCHUNK) & (i < 2 * NCHUNK))
        def _():
            relay2(1, i - NCHUNK)

        return 0

    lax.fori_loop(0, dtiles // 2, dense_b, 0)

    y2_store(dtiles - 2, 0).wait()
    y2_store(dtiles - 1, 1).wait()
    for k in range(1, n):
        mx_msg(k).wait_send()
        z_msg(k).wait_send()

    def drain(c, _):
        for g in range(NGRP):
            for kind in range(7):
                rs(kind, g, c).wait_send()
            for kind in range(9):
                ag(kind, g, c).wait_send()
            own_copy(g, c).wait()
            for kind in (OPA, PUP, PDN, PLO, PHI):
                ag(kind, g, c).wait_recv()
        return 0

    lax.fori_loop(0, NCHUNK, drain, 0)


def combine_kernel(g_ref, mix_ref, y2_ref, y_ref):
    pairs = g_ref.shape[3]
    cols = mix_ref.shape[1]
    rows = mix_ref.shape[0] // pairs

    def body(p, _):
        sl = pl.ds(pl.multiple_of(p * rows, rows), rows)
        rhs = g_ref[:, :, :, p].reshape(cols, g_ref.shape[5])
        y_ref[sl, :] = (dot(mix_ref[sl, :], rhs) + y2_ref[sl, :]).astype(BF16)
        return 0

    lax.fori_loop(0, pairs, body, 0)


def solution(mesh):
    n = mesh.shape['seq']
    chips = n // 2
    tok_spec = P('data', 'seq', None)
    expert_spec = P('seq', None, None)

    def per_device(x_blk, len_blk, phi_slots, scale_g, w_in_blk, w_out_blk, ws_in, ws_out):
        batch, tok, width = x_blk.shape
        slots = phi_slots.shape[1]
        hidden = ws_in.shape[1]
        cols = 2 * slots
        npair = batch // 2
        ntok = batch * tok
        x2 = x_blk.reshape(ntok, width)
        phi_norm = (scale_g * unit_rows(phi_slots, 0)).astype(BF16)
        phi_cols = phi_norm.reshape(width, chips, 2, NGRP, ER).transpose(0, 3, 2, 1, 4)
        phi_cols = jnp.broadcast_to(phi_cols[:, :, :, :, None, :], (width, NGRP, 2, chips, 2, ER)).reshape(width, cols)

        fb = 4
        ft = ntok // fb
        xn, lm, mix, pm = pl.pallas_call(
            functools.partial(front_kernel, tok),
            grid_spec=pltpu.PrefetchScalarGridSpec(
                num_scalar_prefetch=1,
                grid=(fb,),
                in_specs=[pl.BlockSpec((ft, width), lambda i, l: (i, 0)),
                          pl.BlockSpec((width, cols), lambda i, l: (0, 0))],
                out_specs=[pl.BlockSpec((ft, width), lambda i, l: (i, 0)),
                           pl.BlockSpec((ft, cols), lambda i, l: (i, 0)),
                           pl.BlockSpec((ft, cols), lambda i, l: (i, 0)),
                           pl.BlockSpec((npair // fb, cols), lambda i, l: (i, 0))]),
            out_shape=[jax.ShapeDtypeStruct((ntok, width), BF16),
                       jax.ShapeDtypeStruct((ntok, cols), F32),
                       jax.ShapeDtypeStruct((ntok, cols), BF16),
                       jax.ShapeDtypeStruct((npair, cols), F32)],
            name='front',
        )(len_blk, x2, phi_cols)

        pc = npair // NCHUNK
        rows = 2 * tok
        dtok = ntok // 16
        any_spec = pl.BlockSpec(memory_space=pl.ANY)
        sem = pltpu.SemaphoreType.DMA
        slot_out, y2 = pl.pallas_call(
            functools.partial(mega_kernel, n),
            in_specs=[any_spec, any_spec, any_spec, pl.BlockSpec(memory_space=pltpu.VMEM),
                      any_spec, any_spec, any_spec, any_spec],
            out_specs=[any_spec, any_spec],
            out_shape=[jax.ShapeDtypeStruct((NGRP, 2, chips, npair, 16, width), BF16),
                       jax.ShapeDtypeStruct((ntok, width), F32)],
            scratch_shapes=[
                pltpu.VMEM((NGRP, 2, chips, npair, 16, width), BF16),
                pltpu.VMEM((NGRP, chips, npair, 16, width), BF16),
                pltpu.VMEM((2, NGRP, npair // 2, 16, width), BF16),
                pltpu.VMEM((2, NGRP, npair, 16, width), BF16),
                pltpu.VMEM((width, hidden), BF16),
                pltpu.VMEM((hidden, width), BF16),
                pltpu.VMEM((2, width, hidden), BF16),
                pltpu.VMEM((2, hidden, width), BF16),
                pltpu.VMEM((2, pc * rows, width), BF16),
                pltpu.VMEM((2, pc * rows, cols), F32),
                pltpu.VMEM((2, dtok, width), BF16),
                pltpu.VMEM((2, dtok, width), F32),
                pltpu.VMEM((width // LANES, npair * 16, LANES), F32),
                pltpu.VMEM((NGRP, npair, 16, width), BF16),
                pltpu.VMEM((n, npair, cols), F32),
                pltpu.VMEM((npair, cols), F32),
                pltpu.VMEM((LANES, cols // 2), F32),
                pltpu.VMEM((2, chips, 16, LANES), F32),
                pltpu.VMEM((n, 16, LANES), F32),
                pltpu.VMEM((16, LANES), F32),
                sem((7, NGRP, NCHUNK)), sem((7, NGRP, NCHUNK)),
                sem((9, NGRP, NCHUNK)), sem((9, NGRP, NCHUNK)),
                sem((n - 1,)), sem((n - 1,)), sem((n - 1,)), sem((n - 1,)),
                sem((2, 2)), sem((2,)), sem((2, 2)), sem((2,)), sem((2,)), sem((NGRP, NCHUNK)),
            ],
            compiler_params=pltpu.CompilerParams(collective_id=0, has_side_effects=True,
                                                 vmem_limit_bytes=VMEM_BYTES),
            name='mega',
        )(x2, lm, xn, pm, ws_in, ws_out, w_in_blk, w_out_blk)

        cb = 8
        ct = ntok // cb
        y = pl.pallas_call(
            combine_kernel,
            grid=(cb,),
            in_specs=[pl.BlockSpec((NGRP, 2, chips, npair // cb, 16, width), lambda i: (0, 0, 0, i, 0, 0)),
                      pl.BlockSpec((ct, cols), lambda i: (i, 0)),
                      pl.BlockSpec((ct, width), lambda i: (i, 0))],
            out_specs=pl.BlockSpec((ct, width), lambda i: (i, 0)),
            out_shape=jax.ShapeDtypeStruct((ntok, width), BF16),
            name='combine',
        )(slot_out, mix, y2)
        return y.reshape(batch, tok, width)

    return jax.shard_map(per_device, mesh=mesh, in_specs=(tok_spec, P('data'), P(), P(), expert_spec, expert_spec, P(), P()), out_specs=tok_spec, check_vma=False)
```

```python
import functools

import jax
import jax.numpy as jnp
from jax import lax
from jax.experimental import pallas as pl
from jax.experimental.pallas import tpu as pltpu
from jax.sharding import PartitionSpec as P

NORM_EPS = 1e-6
NEG_BIG = -1e30
F32 = jnp.float32
BF16 = jnp.bfloat16
MESH = pl.DeviceIdType.MESH
LANES = 128
NGRP = 2
NCHUNK = 4
ER = 8
VMEM_BYTES = 67043328
UNROLL = 4
DTOK = 256
DENSE_A = 6
DENSE_E = ()

D2D, TUP, TDN, RUP, RDN, SUP, SDN = range(7)
OUP, ODN, OPA, FUP, FDN, PUP, PDN, PLO, PHI = range(9)


def unit_rows(values, axis_id):
    wide_vals = values.astype(F32)
    return wide_vals / jnp.sqrt(jnp.sum(wide_vals * wide_vals, axis=axis_id, keepdims=True) + NORM_EPS)


def dot(a, b):
    return jnp.dot(a, b, preferred_element_type=F32)


def gelu(v):
    return jax.nn.gelu(v, approximate=True)


def mega_kernel(n, tok, len_ref, phi, x_hbm, wsi_hbm, wso_hbm, w1_hbm, w2_hbm,
                y_hbm, y2_hbm, xn_hbm,
                part, dbuf, tbuf, rbuf, wsi, wso, w1b, w2b, lb, mixb, xnb, y2b, y2c, yt, sbuf,
                pm, mxb, mx, zs, zt, zb, zo,
                rs_s, rs_r, ag_s, ag_r, mx_s, mx_r, z_s, z_r, x_sem, xs_sem, ws_sem, w_sem, xn_sem, y2_sem,
                yc_sem, yt_sem, free_sem):
    me = lax.axis_index('seq')
    chip, core = me // 2, me % 2
    chips = n // 2
    mate = chip * 2 + (1 - core)
    cup, cdn, cop = (chip + 1) % chips, (chip + chips - 1) % chips, (chip + 2) % chips
    up, dn = cup * 2 + core, cdn * 2 + core
    npair, cols = pm.shape
    pc = npair // NCHUNK
    ph = pc // 2
    rows = 2 * tok
    crows = pc * rows
    dwidth = phi.shape[0]
    ntile = dwidth // LANES
    dtiles = y2_hbm.shape[0] // DTOK
    per = w2b.shape[1] // crows

    def rdma(src, dst, ss, rs, dev):
        return pltpu.make_async_remote_copy(src_ref=src, dst_ref=dst, send_sem=ss, recv_sem=rs,
                                            device_id={'seq': dev}, device_id_type=MESH)

    def w2_rows(block, off, size):
        return block // per, pl.ds(pl.multiple_of((block % per) * crows + off, rows), size)

    def tok_rows(c):
        return pl.ds(pl.multiple_of(c * crows, crows), crows)

    def x_load(c):
        b, sl = w2_rows(c, 0, crows)
        return pltpu.make_async_copy(x_hbm.at[tok_rows(c), :], w2b.at[b, sl, :], x_sem.at[c])

    def xn_store(c):
        b, sl = w2_rows(NCHUNK + c % 2, 0, crows)
        return pltpu.make_async_copy(w2b.at[b, sl, :], xn_hbm.at[tok_rows(c), :], xs_sem.at[c % 2])

    def w_load(e, slot):
        return (pltpu.make_async_copy(w1_hbm.at[e], w1b.at[slot], w_sem.at[0, slot]),
                pltpu.make_async_copy(w2_hbm.at[e], w2b.at[slot], w_sem.at[1, slot]))

    def ws_load():
        return (pltpu.make_async_copy(wsi_hbm, wsi, ws_sem.at[0]),
                pltpu.make_async_copy(wso_hbm, wso, ws_sem.at[1]))

    def tile_rows(i):
        return pl.ds(pl.multiple_of(i * DTOK, DTOK), DTOK)

    def xn_load(i, slot):
        return pltpu.make_async_copy(xn_hbm.at[tile_rows(i), :], xnb.at[slot], xn_sem.at[slot])

    def y2_store(i, slot):
        return pltpu.make_async_copy(y2b.at[slot], y2_hbm.at[tile_rows(i), :], y2_sem.at[slot])

    def y2_load(i, slot):
        return pltpu.make_async_copy(y2_hbm.at[tile_rows(i), :], y2c.at[slot], yc_sem.at[slot])

    def y_store(i, slot):
        return pltpu.make_async_copy(yt.at[slot], y_hbm.at[tile_rows(i), :], yt_sem.at[slot])

    def start(copies):
        for cp in copies:
            cp.start()

    def side_by_side(count, one):
        def body(i, _):
            for u in range(UNROLL):
                one(i * UNROLL + u)
            return 0

        lax.fori_loop(0, count // UNROLL, body, 0)

    def all_of(c):
        return pl.ds(c * pc, pc)

    def lo_of(c):
        return pl.ds(c * pc, ph)

    def hi_of(c):
        return pl.ds(c * pc + ph, ph)

    def rs(kind, g, c):
        ss, rr = rs_s.at[kind, g, c], rs_r.at[kind, g, c]
        mine = part.at[g, core]
        if kind == D2D:
            return rdma(part.at[g, 1 - core, :, all_of(c)], dbuf.at[g, :, all_of(c)], ss, rr, mate)
        if kind == TUP:
            return rdma(mine.at[cop, lo_of(c)], tbuf.at[0, g, pl.ds(c * ph, ph)], ss, rr, up)
        if kind == TDN:
            return rdma(mine.at[cop, hi_of(c)], tbuf.at[1, g, pl.ds(c * ph, ph)], ss, rr, dn)
        if kind == RUP:
            return rdma(mine.at[cup, hi_of(c)], rbuf.at[0, g, hi_of(c)], ss, rr, up)
        if kind == RDN:
            return rdma(mine.at[cdn, lo_of(c)], rbuf.at[1, g, lo_of(c)], ss, rr, dn)
        if kind == SUP:
            return rdma(mine.at[cup, lo_of(c)], rbuf.at[0, g, lo_of(c)], ss, rr, up)
        return rdma(mine.at[cdn, hi_of(c)], rbuf.at[1, g, hi_of(c)], ss, rr, dn)

    def stage1(g, c):
        rs(D2D, g, c).wait_recv()

        def body(i, _):
            q = c * pc + i
            a = part[g, core, :, q].astype(F32) + dbuf[g, :, q].astype(F32)
            part[g, core, :, q] = a.astype(BF16)
            return 0

        lax.fori_loop(0, pc, body, 0)
        for kind in (TUP, TDN, RUP, RDN):
            rs(kind, g, c).start()

    def stage2(g, c):
        for kind, nxt, dst, off, d in ((TUP, SUP, cup, 0, 0), (TDN, SDN, cdn, ph, 1)):
            rs(kind, g, c).wait_recv()

            def body(i, _):
                q = c * pc + off + i
                a = part[g, core, dst, q].astype(F32) + tbuf[d, g, c * ph + i].astype(F32)
                part[g, core, dst, q] = a.astype(BF16)
                return 0

            lax.fori_loop(0, ph, body, 0)
            rs(nxt, g, c).start()

    def stage3(g, c):
        for kind in (RUP, RDN, SUP, SDN):
            rs(kind, g, c).wait_recv()
        zg = zo[...]
        lane = lax.broadcasted_iota(jnp.int32, zg.shape, 1)

        def one(i):
            q = c * pc + i
            z = jnp.sum(jnp.where(lane == g * npair + q, zg, 0.0), axis=1, keepdims=True)
            a = part[g, core, chip, q].astype(F32) + rbuf[0, g, q].astype(F32) + rbuf[1, g, q].astype(F32)
            a = a / z
            for j in range(ntile):
                sbuf[j, pl.ds(pl.multiple_of(q * 16, 16), 16), :] = a[:, j * LANES:(j + 1) * LANES]

        side_by_side(pc, one)

    def run3(g):
        def body(c, _):
            stage3(g, c)
            return 0

        lax.fori_loop(0, NCHUNK, body, 0)

        def sent(c, _):
            for kind in range(7):
                rs(kind, g, c).wait_send()
            return 0

        lax.fori_loop(0, NCHUNK, sent, 0)
        for dev in (up, dn, mate):
            pl.semaphore_signal(free_sem.at[g], inc=1, device_id={'seq': dev}, device_id_type=MESH)

    def ag(kind, g, c):
        origin, part_of, dev = {OUP: (chip, all_of, up), ODN: (chip, all_of, dn), OPA: (chip, all_of, mate),
                                FUP: (cdn, lo_of, up), FDN: (cup, hi_of, dn),
                                PUP: (cdn, all_of, mate), PDN: (cup, all_of, mate),
                                PLO: (cop, lo_of, mate), PHI: (cop, hi_of, mate)}[kind]
        ref = part.at[g, core, origin, part_of(c)]
        return rdma(ref, ref, ag_s.at[kind, g, c], ag_r.at[kind, g, c], dev)

    def send_own(g, c):
        for kind in (OUP, ODN, OPA):
            ag(kind, g, c).start()

    def pack(g):
        def body(q, _):
            for j in range(ntile):
                part[g, core, chip, q, :, j * LANES:(j + 1) * LANES] = (
                    sbuf[j, pl.ds(pl.multiple_of(q * 16, 16), 16), :].astype(BF16))
            return 0

        lax.fori_loop(0, npair, body, 0)
        pl.semaphore_wait(free_sem.at[g], 3)

    def relay1(g, c):
        ag(OUP, g, c).wait_recv()
        ag(FUP, g, c).start()
        ag(PUP, g, c).start()
        ag(ODN, g, c).wait_recv()
        ag(FDN, g, c).start()
        ag(PDN, g, c).start()

    def relay2(g, c):
        ag(FUP, g, c).wait_recv()
        ag(PLO, g, c).start()
        ag(FDN, g, c).wait_recv()
        ag(PHI, g, c).start()

    def front(c):
        x_load(c).wait()

        @pl.when(c >= 2)
        def _():
            xn_store(c - 2).wait()

        first = me * tok

        def one(p):
            q = c * pc + p
            b, sl = w2_rows(c, p * rows, rows)
            x = w2b[b, sl, :].astype(F32)
            inv = lax.rsqrt(jnp.sum(x * x, axis=1, keepdims=True) + NORM_EPS)
            xn = (x * inv).astype(BF16)
            b, sl = w2_rows(NCHUNK + c % 2, p * rows, rows)
            w2b[b, sl, :] = xn
            logits = dot(xn, phi[...])
            ri = lax.broadcasted_iota(jnp.int32, (rows, cols), 0)
            ci = lax.broadcasted_iota(jnp.int32, (rows, cols), 1)
            odd = ri >= tok
            same = jnp.where(odd, 1, 0) == ((ci >> 3) & 1)
            lim = jnp.where(odd, len_ref[2 * q + 1], len_ref[2 * q])
            valid = (first + (ri & (tok - 1))) < lim
            own = jnp.where(same, logits, NEG_BIG)
            top = jnp.max(own, axis=1, keepdims=True)
            ex = jnp.exp(own - top)
            mixb[pl.ds(pl.multiple_of(q * rows, rows), rows), :] = (
                ex * (1.0 / jnp.sum(ex, axis=1, keepdims=True))).astype(BF16)
            lm = jnp.where(valid, own, NEG_BIG)
            lb[c % 2, pl.ds(pl.multiple_of(p * rows, rows), rows), :] = lm
            pm[pl.ds(q, 1), :] = jnp.max(lm, axis=0, keepdims=True)

        side_by_side(pc, one)
        xn_store(c).start()

    def mx_msg(k, c):
        sl = pl.ds(pl.multiple_of(c * pc, pc), pc)
        return rdma(pm.at[sl, :], mxb.at[me, sl, :], mx_s.at[k - 1, c], mx_r.at[k - 1, c], lax.rem(me + k, n))

    half = cols // 2

    def numerators(c):
        sl = pl.ds(pl.multiple_of(c * pc, pc), pc)
        for k in range(1, n):
            mx_msg(k, c).wait_recv()
        top = pm[sl, :]
        for k in range(1, n):
            top = jnp.maximum(top, mxb[lax.rem(me + n - k, n), sl, :])
        mx[sl, :] = top

        def one(p):
            q = c * pc + p
            e = jnp.exp(lb[c % 2, pl.ds(pl.multiple_of(p * rows, rows), rows), :] - mx[pl.ds(q, 1), :])
            z = jnp.sum(e, axis=0, keepdims=True)
            zs[pl.ds(q, 1), :] = z[:, :half]
            zs[pl.ds(npair + q, 1), :] = z[:, half:]
            b, xsl = w2_rows(c, p * rows, rows)
            num = lax.dot_general(e.astype(BF16), w2b[b, xsl, :], (((0,), (0,)), ((), ())),
                                  preferred_element_type=F32)
            part[:, :, :, q] = num.astype(BF16).reshape(NGRP, 2, chips, 16, dwidth)

        side_by_side(pc, one)
        for g in range(NGRP):
            rs(D2D, g, c).start()

    def dense_tile(i):
        slot = i % 2
        xn_load(i, slot).wait()
        xt = xnb[slot]
        hidden = wsi.shape[1]
        step = min(hidden, 768)
        acc = None
        for f in range(0, hidden, step):
            h = gelu(dot(xt, wsi[:, f:f + step])).astype(BF16)
            o = dot(h, wso[f:f + step, :])
            acc = o if acc is None else acc + o

        @pl.when(i >= 2)
        def _():
            y2_store(i - 2, slot).wait()

        y2b[slot] = acc
        y2_store(i, slot).start()

        @pl.when(i + 2 < dtiles)
        def _():
            xn_load(i + 2, slot).start()

    def expert(g, e, total):
        idx = g * ER + e
        slot = idx % 2
        xin = jnp.concatenate([sbuf[j, pl.ds(e, 2 * npair, stride=ER), :] for j in range(ntile)], axis=1).astype(BF16)
        l1, l2 = w_load(idx, slot)
        l1.wait()
        l2.wait()
        hidden = w1b.shape[2]
        step = min(hidden, 768)
        acc = None
        for f in range(0, hidden, step):
            h = gelu(dot(xin, w1b[slot, :, f:f + step])).astype(BF16)
            o = dot(h, w2b[slot, f:f + step, :])
            acc = o if acc is None else acc + o
        for j in range(ntile):
            sbuf[j, pl.ds(e, 2 * npair, stride=ER), :] = acc[:, j * LANES:(j + 1) * LANES]

        @pl.when(idx + 2 < total)
        def _():
            start(w_load(idx + 2, slot))

    def combine(c):
        tiles = crows // DTOK
        first = c * tiles
        y2_load(first, 0).start()
        y2_load(first + 1, 1).start()
        for g in range(NGRP):
            for kind in (OPA, PUP, PDN, PLO, PHI):
                ag(kind, g, c).wait_recv()
        for t in range(tiles):
            i, slot = first + t, t % 2
            y2_load(i, slot).wait()
            if c > 0 or t >= 2:
                y_store(i - 2, slot).wait()
            for u in range(DTOK // rows):
                q = i * (DTOK // rows) + u
                lr = slice(u * rows, (u + 1) * rows)
                rhs = part[:, :, :, q].reshape(cols, dwidth)
                yt[slot, lr, :] = (dot(mixb[q * rows:(q + 1) * rows, :], rhs) + y2c[slot, lr, :]).astype(BF16)
            y_store(i, slot).start()
            if t + 2 < tiles:
                y2_load(i + 2, slot).start()

    for c in range(NCHUNK):
        x_load(c).start()
    start(ws_load())
    barrier = pltpu.get_barrier_semaphore()
    for k in range(1, n):
        pl.semaphore_signal(barrier, inc=1, device_id={'seq': lax.rem(me + k, n)}, device_id_type=MESH)
    zs[...] = jnp.zeros_like(zs)
    pl.semaphore_wait(barrier, n - 1)

    def opening(s, _):
        @pl.when(s < NCHUNK)
        def _():
            front(s)
            for k in range(1, n):
                mx_msg(k, s).start()

        @pl.when(s == 2)
        def _():
            xn_load(0, 0).start()
            xn_load(1, 1).start()

        @pl.when(s == NCHUNK)
        def _():
            for cp in ws_load():
                cp.wait()

        @pl.when(s >= NCHUNK)
        def _():
            dense_tile(s - NCHUNK)

        @pl.when(s >= 2)
        def _():
            stage1(0, s - 2)

        @pl.when((s >= 1) & (s <= NCHUNK))
        def _():
            numerators(s - 1)

        return 0

    lax.fori_loop(0, NCHUNK + 2, opening, 0)
    for c in (NCHUNK - 2, NCHUNK - 1):
        xn_store(c).wait()
    start(w_load(0, 0))
    start(w_load(1, 1))

    zt[...] = zs[...].T.reshape(zt.shape)

    def z_msg(k):
        dev = lax.rem(me + k, n)
        return rdma(zt.at[dev % 2, dev // 2], zb.at[me], z_s.at[k - 1], z_r.at[k - 1], dev)

    for k in range(1, n):
        z_msg(k).start()

    def dense_a(i, _):
        dense_tile(2 + i)

        @pl.when(i < NCHUNK)
        def _():
            stage2(0, i)

        return 0

    lax.fori_loop(0, DENSE_A - 2, dense_a, 0)

    def next1(c, _):
        stage1(1, c)
        return 0

    lax.fori_loop(0, NCHUNK, next1, 0)
    for k in range(1, n):
        z_msg(k).wait_recv()
    ztot = zt[core, chip]
    for k in range(1, n):
        ztot = ztot + zb[lax.rem(me + n - k, n)]
    zo[...] = ztot
    run3(0)

    total = NGRP * ER

    def experts_a(e, _):
        expert(0, e, total)

        @pl.when(e < NCHUNK)
        def _():
            stage2(1, e)

        for k, at in enumerate(DENSE_E):
            @pl.when(e == at)
            def _():
                dense_tile(DENSE_A + k)

        return 0

    lax.fori_loop(0, ER, experts_a, 0)
    pack(0)
    for c in range(NCHUNK):
        send_own(0, c)
    run3(1)

    def experts_b(e, _):
        expert(1, e, total)

        @pl.when(e < NCHUNK)
        def _():
            relay1(0, e)

        @pl.when(e >= NCHUNK)
        def _():
            relay2(0, e - NCHUNK)

        for k, at in enumerate(DENSE_E):
            @pl.when(e == at)
            def _():
                dense_tile(DENSE_A + len(DENSE_E) + k)

        return 0

    lax.fori_loop(0, ER, experts_b, 0)
    pack(1)
    send_own(1, 0)
    send_own(1, 1)

    before = DENSE_A + 2 * len(DENSE_E)
    count = dtiles - before
    events = ((2, relay1, 0), (2, send_own, 2), (4, relay1, 1), (4, send_own, 3), (5, relay2, 0),
              (7, relay1, 2), (7, relay2, 1), (8, None, 0), (99, relay1, 3), (99, relay2, 2), (99, None, 1), (99, None, 2),
              (99, relay2, 3), (99, None, 3))

    def run(at, what, c):
        if what is None:
            combine(c)
        else:
            what(1, c)

    def dense_b(i, _):
        dense_tile(before + i)
        for at, what, c in events:
            if at < count:
                @pl.when(i == at)
                def _():
                    run(at, what, c)
        return 0

    lax.fori_loop(0, count, dense_b, 0)
    y2_store(dtiles - 2, (dtiles - 2) % 2).wait()
    y2_store(dtiles - 1, (dtiles - 1) % 2).wait()
    for at, what, c in events:
        if at >= count:
            run(at, what, c)

    y_store(dtiles - 2, 0).wait()
    y_store(dtiles - 1, 1).wait()
    for k in range(1, n):
        z_msg(k).wait_send()

    def drain(c, _):
        for k in range(1, n):
            mx_msg(k, c).wait_send()
        for g in range(NGRP):
            for kind in range(9):
                ag(kind, g, c).wait_send()
        return 0

    lax.fori_loop(0, NCHUNK, drain, 0)


def solution(mesh):
    n = mesh.shape['seq']
    chips = n // 2
    tok_spec = P('data', 'seq', None)
    expert_spec = P('seq', None, None)

    def per_device(x_blk, len_blk, phi_slots, scale_g, w_in_blk, w_out_blk, ws_in, ws_out):
        batch, tok, width = x_blk.shape
        slots = phi_slots.shape[1]
        hidden = ws_in.shape[1]
        cols = 2 * slots
        npair = batch // 2
        ntok = batch * tok
        x2 = x_blk.reshape(ntok, width)
        phi_norm = (scale_g * unit_rows(phi_slots, 0)).astype(BF16)
        phi_cols = phi_norm.reshape(width, chips, 2, NGRP, ER).transpose(0, 3, 2, 1, 4)
        phi_cols = jnp.broadcast_to(phi_cols[:, :, :, :, None, :], (width, NGRP, 2, chips, 2, ER)).reshape(width, cols)

        pc = npair // NCHUNK
        rows = 2 * tok
        any_spec = pl.BlockSpec(memory_space=pl.ANY)
        sem = pltpu.SemaphoreType.DMA
        y, _, _ = pl.pallas_call(
            functools.partial(mega_kernel, n, tok),
            in_specs=[pl.BlockSpec(memory_space=pltpu.SMEM), pl.BlockSpec(memory_space=pltpu.VMEM),
                      any_spec, any_spec, any_spec, any_spec, any_spec],
            out_specs=[any_spec, any_spec, any_spec],
            out_shape=[jax.ShapeDtypeStruct((ntok, width), BF16),
                       jax.ShapeDtypeStruct((ntok, width), F32),
                       jax.ShapeDtypeStruct((ntok, width), BF16)],
            scratch_shapes=[
                pltpu.VMEM((NGRP, 2, chips, npair, 16, width), BF16),
                pltpu.VMEM((NGRP, chips, npair, 16, width), BF16),
                pltpu.VMEM((2, NGRP, npair // 2, 16, width), BF16),
                pltpu.VMEM((2, NGRP, npair, 16, width), BF16),
                pltpu.VMEM((width, hidden), BF16),
                pltpu.VMEM((hidden, width), BF16),
                pltpu.VMEM((2, width, hidden), BF16),
                pltpu.VMEM((2, hidden, width), BF16),
                pltpu.VMEM((2, pc * rows, cols), F32),
                pltpu.VMEM((ntok, cols), BF16),
                pltpu.VMEM((2, DTOK, width), BF16),
                pltpu.VMEM((2, DTOK, width), F32),
                pltpu.VMEM((2, DTOK, width), F32),
                pltpu.VMEM((2, DTOK, width), BF16),
                pltpu.VMEM((width // LANES, npair * 16, LANES), F32),
                pltpu.VMEM((npair, cols), F32),
                pltpu.VMEM((n, npair, cols), F32),
                pltpu.VMEM((npair, cols), F32),
                pltpu.VMEM((LANES, cols // 2), F32),
                pltpu.VMEM((2, chips, 16, LANES), F32),
                pltpu.VMEM((n, 16, LANES), F32),
                pltpu.VMEM((16, LANES), F32),
                sem((7, NGRP, NCHUNK)), sem((7, NGRP, NCHUNK)),
                sem((9, NGRP, NCHUNK)), sem((9, NGRP, NCHUNK)),
                sem((n - 1, NCHUNK)), sem((n - 1, NCHUNK)), sem((n - 1,)), sem((n - 1,)),
                sem((NCHUNK,)), sem((2,)), sem((2,)), sem((2, 2)), sem((2,)), sem((2,)),
                sem((2,)), sem((2,)), pltpu.SemaphoreType.REGULAR((NGRP,)),
            ],
            compiler_params=pltpu.CompilerParams(collective_id=0, has_side_effects=True,
                                                 vmem_limit_bytes=VMEM_BYTES),
            name='mega',
        )(len_blk, phi_cols, x2, ws_in, ws_out, w_in_blk, w_out_blk)
        return y.reshape(batch, tok, width)

    return jax.shard_map(per_device, mesh=mesh, in_specs=(tok_spec, P('data'), P(), P(), expert_spec, expert_spec, P(), P()), out_specs=tok_spec, check_vma=False)
```

```python
import functools

import jax
import jax.numpy as jnp
import numpy as np
from jax import lax
from jax.experimental import pallas as pl
from jax.experimental.pallas import tpu as pltpu
from jax.sharding import PartitionSpec as P

NORM_EPS = 1e-6
NEG_BIG = -1e30
F32 = jnp.float32
BF16 = jnp.bfloat16
MESH = pl.DeviceIdType.MESH
LANES = 128
NGRP = 2
NCHUNK = 4
ER = 8
VMEM_BYTES = 67043328
UNROLL = 4
DTOK = 256
DENSE_A = 5

D2D, TUP, TDN, RUP, RDN, SUP, SDN = range(7)
OUP, ODN, OPA, FUP, FDN, PUP, PDN, PLO, PHI = range(9)


def unit_rows(values, axis_id):
    wide_vals = values.astype(F32)
    return wide_vals / jnp.sqrt(jnp.sum(wide_vals * wide_vals, axis=axis_id, keepdims=True) + NORM_EPS)


def dot(a, b):
    return jnp.dot(a, b, preferred_element_type=F32)


def gelu(v):
    return jax.nn.gelu(v, approximate=True)


def mega_kernel(n, tok, len_ref, gain_ref, phi_ref, perm_ref, x_hbm, wsi_hbm, wso_hbm, w1_hbm, w2_hbm,
                y_hbm, y2_hbm, xn_hbm,
                part, dbuf, tbuf, rbuf, wsi, wso, w1b, w2b, mixb, xnb, y2b, y2c, yt, sbuf,
                phi, pm, mxb, mx, zs, zt, zb, zo,
                rs_s, rs_r, ag_s, ag_r, mx_s, mx_r, z_s, z_r, x_sem, xs_sem, ws_sem, w_sem, xn_sem, y2_sem,
                yc_sem, yt_sem, free_sem):
    me = lax.axis_index('seq')
    chip, core = me // 2, me % 2
    chips = n // 2
    mate = chip * 2 + (1 - core)
    cup, cdn, cop = (chip + 1) % chips, (chip + chips - 1) % chips, (chip + 2) % chips
    up, dn = cup * 2 + core, cdn * 2 + core
    npair, cols = pm.shape
    pc = npair // NCHUNK
    ph = pc // 2
    rows = 2 * tok
    crows = pc * rows
    dwidth = phi.shape[0]
    tiles = crows // DTOK
    ntile = dwidth // LANES
    dtiles = y2_hbm.shape[0] // DTOK
    per = w2b.shape[1] // crows

    def rdma(src, dst, ss, rs, dev):
        return pltpu.make_async_remote_copy(src_ref=src, dst_ref=dst, send_sem=ss, recv_sem=rs,
                                            device_id={'seq': dev}, device_id_type=MESH)

    def w2_rows(block, off, size):
        return block // per, pl.ds(pl.multiple_of((block % per) * crows + off, rows), size)

    def tok_rows(c):
        return pl.ds(pl.multiple_of(c * crows, crows), crows)

    def x_load(c):
        b, sl = w2_rows(c, 0, crows)
        return pltpu.make_async_copy(x_hbm.at[tok_rows(c), :], w2b.at[b, sl, :], x_sem.at[c])

    def xn_store(c):
        b, sl = w2_rows(NCHUNK + c % 2, 0, crows)
        return pltpu.make_async_copy(w2b.at[b, sl, :], xn_hbm.at[tok_rows(c), :], xs_sem.at[c % 2])

    def w_load(e, slot):
        return (pltpu.make_async_copy(w1_hbm.at[e], w1b.at[slot], w_sem.at[0, slot]),
                pltpu.make_async_copy(w2_hbm.at[e], w2b.at[slot], w_sem.at[1, slot]))

    def ws_load():
        return (pltpu.make_async_copy(wsi_hbm, wsi, ws_sem.at[0]),
                pltpu.make_async_copy(wso_hbm, wso, ws_sem.at[1]))

    def tile_rows(i):
        return pl.ds(pl.multiple_of(i * DTOK, DTOK), DTOK)

    def xn_load(i, slot):
        return pltpu.make_async_copy(xn_hbm.at[tile_rows(i), :], xnb.at[slot], xn_sem.at[slot])

    def y2_store(i, slot):
        return pltpu.make_async_copy(y2b.at[slot], y2_hbm.at[tile_rows(i), :], y2_sem.at[slot])

    def y2_load(i, slot):
        return pltpu.make_async_copy(y2_hbm.at[tile_rows(i), :], y2c.at[slot], yc_sem.at[slot])

    def y_store(i, slot):
        return pltpu.make_async_copy(yt.at[slot], y_hbm.at[tile_rows(i), :], yt_sem.at[slot])

    def start(copies):
        for cp in copies:
            cp.start()

    def side_by_side(count, one):
        def body(i, _):
            for u in range(UNROLL):
                one(i * UNROLL + u)
            return 0

        lax.fori_loop(0, count // UNROLL, body, 0)

    def all_of(c):
        return pl.ds(c * pc, pc)

    def lo_of(c):
        return pl.ds(c * pc, ph)

    def hi_of(c):
        return pl.ds(c * pc + ph, ph)

    def rs(kind, g, c):
        ss, rr = rs_s.at[kind, g, c], rs_r.at[kind, g, c]
        mine = part.at[g, core]
        if kind == D2D:
            return rdma(part.at[g, 1 - core, :, all_of(c)], dbuf.at[g, :, all_of(c)], ss, rr, mate)
        if kind == TUP:
            return rdma(mine.at[cop, lo_of(c)], tbuf.at[0, g, pl.ds(c * ph, ph)], ss, rr, up)
        if kind == TDN:
            return rdma(mine.at[cop, hi_of(c)], tbuf.at[1, g, pl.ds(c * ph, ph)], ss, rr, dn)
        if kind == RUP:
            return rdma(mine.at[cup, hi_of(c)], rbuf.at[0, g, hi_of(c)], ss, rr, up)
        if kind == RDN:
            return rdma(mine.at[cdn, lo_of(c)], rbuf.at[1, g, lo_of(c)], ss, rr, dn)
        if kind == SUP:
            return rdma(mine.at[cup, lo_of(c)], rbuf.at[0, g, lo_of(c)], ss, rr, up)
        return rdma(mine.at[cdn, hi_of(c)], rbuf.at[1, g, hi_of(c)], ss, rr, dn)

    def stage1(g, c):
        rs(D2D, g, c).wait_recv()

        def body(i, _):
            q = c * pc + i
            a = part[g, core, :, q].astype(F32) + dbuf[g, :, q].astype(F32)
            part[g, core, :, q] = a.astype(BF16)
            return 0

        lax.fori_loop(0, pc, body, 0)
        for kind in (TUP, TDN, RUP, RDN):
            rs(kind, g, c).start()

    def stage2(g, c):
        for kind, nxt, dst, off, d in ((TUP, SUP, cup, 0, 0), (TDN, SDN, cdn, ph, 1)):
            rs(kind, g, c).wait_recv()

            def body(i, _):
                q = c * pc + off + i
                a = part[g, core, dst, q].astype(F32) + tbuf[d, g, c * ph + i].astype(F32)
                part[g, core, dst, q] = a.astype(BF16)
                return 0

            lax.fori_loop(0, ph, body, 0)
            rs(nxt, g, c).start()

    def stage3(g, c):
        for kind in (RUP, RDN, SUP, SDN):
            rs(kind, g, c).wait_recv()
        zg = zo[...]
        lane = lax.broadcasted_iota(jnp.int32, zg.shape, 1)

        def one(i):
            q = c * pc + i
            z = jnp.sum(jnp.where(lane == g * npair + q, zg, 0.0), axis=1, keepdims=True)
            a = part[g, core, chip, q].astype(F32) + rbuf[0, g, q].astype(F32) + rbuf[1, g, q].astype(F32)
            a = a / z
            for j in range(ntile):
                sbuf[j, pl.ds(pl.multiple_of(q * 16, 16), 16), :] = a[:, j * LANES:(j + 1) * LANES]

        side_by_side(pc, one)

    def run3(g):
        def body(c, _):
            stage3(g, c)
            return 0

        lax.fori_loop(0, NCHUNK, body, 0)

        def sent(c, _):
            for kind in range(7):
                rs(kind, g, c).wait_send()
            return 0

        lax.fori_loop(0, NCHUNK, sent, 0)
        for dev in (up, dn, mate):
            pl.semaphore_signal(free_sem.at[g], inc=1, device_id={'seq': dev}, device_id_type=MESH)

    def ag(kind, g, c):
        origin, part_of, dev = {OUP: (chip, all_of, up), ODN: (chip, all_of, dn), OPA: (chip, all_of, mate),
                                FUP: (cdn, lo_of, up), FDN: (cup, hi_of, dn),
                                PUP: (cdn, all_of, mate), PDN: (cup, all_of, mate),
                                PLO: (cop, lo_of, mate), PHI: (cop, hi_of, mate)}[kind]
        ref = part.at[g, core, origin, part_of(c)]
        return rdma(ref, ref, ag_s.at[kind, g, c], ag_r.at[kind, g, c], dev)

    def send_own(g, c):
        for kind in (OUP, ODN, OPA):
            ag(kind, g, c).start()

    def pack(g):
        def body(q, _):
            for j in range(ntile):
                part[g, core, chip, q, :, j * LANES:(j + 1) * LANES] = (
                    sbuf[j, pl.ds(pl.multiple_of(q * 16, 16), 16), :].astype(BF16))
            return 0

        lax.fori_loop(0, npair, body, 0)
        pl.semaphore_wait(free_sem.at[g], 3)

    def relay1(g, c):
        ag(OUP, g, c).wait_recv()
        ag(FUP, g, c).start()
        ag(PUP, g, c).start()
        ag(ODN, g, c).wait_recv()
        ag(FDN, g, c).start()
        ag(PDN, g, c).start()

    def relay2(g, c):
        ag(FUP, g, c).wait_recv()
        ag(PLO, g, c).start()
        ag(FDN, g, c).wait_recv()
        ag(PHI, g, c).start()

    def logit_at(c, p):
        each = DTOK // rows
        return (p // each, pl.ds(pl.multiple_of(p % each * rows, rows), rows),
                pl.ds(pl.multiple_of(c % (NCHUNK - 1) * cols, cols), cols))

    def front(c):
        x_load(c).wait()

        @pl.when(c >= 2)
        def _():
            xn_store(c - 2).wait()

        first = me * tok

        def one(p):
            q = c * pc + p
            b, sl = w2_rows(c, p * rows, rows)
            x = w2b[b, sl, :].astype(F32)
            inv = lax.rsqrt(jnp.sum(x * x, axis=1, keepdims=True) + NORM_EPS)
            xn = (x * inv).astype(BF16)
            b, sl = w2_rows(NCHUNK + c % 2, p * rows, rows)
            w2b[b, sl, :] = xn
            logits = dot(xn, phi[...])
            ri = lax.broadcasted_iota(jnp.int32, (rows, cols), 0)
            ci = lax.broadcasted_iota(jnp.int32, (rows, cols), 1)
            odd = ri >= tok
            same = jnp.where(odd, 1, 0) == ((ci >> 3) & 1)
            lim = jnp.where(odd, len_ref[2 * q + 1], len_ref[2 * q])
            valid = (first + (ri & (tok - 1))) < lim
            own = jnp.where(same, logits, NEG_BIG)
            top = jnp.max(own, axis=1, keepdims=True)
            ex = jnp.exp(own - top)
            mixb[pl.ds(pl.multiple_of(q * rows, rows), rows), :] = (
                ex * (1.0 / jnp.sum(ex, axis=1, keepdims=True))).astype(BF16)
            lm = jnp.where(valid, own, NEG_BIG)
            t, tr, tc = logit_at(c, p)
            y2c[t, tr, tc] = lm
            pm[pl.ds(q, 1), :] = jnp.max(lm, axis=0, keepdims=True)

        side_by_side(pc, one)
        xn_store(c).start()

    def mx_msg(k, c):
        sl = pl.ds(pl.multiple_of(c * pc, pc), pc)
        return rdma(pm.at[sl, :], mxb.at[me, sl, :], mx_s.at[k - 1, c], mx_r.at[k - 1, c], lax.rem(me + k, n))

    half = cols // 2

    def numerators(c):
        sl = pl.ds(pl.multiple_of(c * pc, pc), pc)
        for k in range(1, n):
            mx_msg(k, c).wait_recv()
        top = pm[sl, :]
        for k in range(1, n):
            top = jnp.maximum(top, mxb[lax.rem(me + n - k, n), sl, :])
        mx[sl, :] = top

        def one(p):
            q = c * pc + p
            t, tr, tc = logit_at(c, p)
            e = jnp.exp(y2c[t, tr, tc] - mx[pl.ds(q, 1), :])
            z = jnp.sum(e, axis=0, keepdims=True)
            zs[pl.ds(q, 1), :] = z[:, :half]
            zs[pl.ds(npair + q, 1), :] = z[:, half:]
            b, xsl = w2_rows(c, p * rows, rows)
            num = lax.dot_general(e.astype(BF16), w2b[b, xsl, :], (((0,), (0,)), ((), ())),
                                  preferred_element_type=F32)
            part[:, :, :, q] = num.astype(BF16).reshape(NGRP, 2, chips, 16, dwidth)

        side_by_side(pc, one)
        for g in range(NGRP):
            rs(D2D, g, c).start()

    def dense_tile(i):
        slot = i % 2
        xn_load(i, slot).wait()
        xt = xnb[slot]
        hidden = wsi.shape[1]
        step = min(hidden, 768)
        acc = None
        for f in range(0, hidden, step):
            h = gelu(dot(xt, wsi[:, f:f + step])).astype(BF16)
            o = dot(h, wso[f:f + step, :])
            acc = o if acc is None else acc + o

        @pl.when(i >= 2)
        def _():
            y2_store(i - 2, slot).wait()

        y2b[slot] = acc
        y2_store(i, slot).start()

        @pl.when(i + 2 < dtiles)
        def _():
            xn_load(i + 2, slot).start()

    def expert(g, e, total):
        idx = g * ER + e
        slot = idx % 2
        xin = jnp.concatenate([sbuf[j, pl.ds(e, 2 * npair, stride=ER), :] for j in range(ntile)], axis=1).astype(BF16)
        l1, l2 = w_load(idx, slot)
        l1.wait()
        l2.wait()
        hidden = w1b.shape[2]
        step = min(hidden, 768)
        acc = None
        for f in range(0, hidden, step):
            h = gelu(dot(xin, w1b[slot, :, f:f + step])).astype(BF16)
            o = dot(h, w2b[slot, f:f + step, :])
            acc = o if acc is None else acc + o
        for j in range(ntile):
            sbuf[j, pl.ds(e, 2 * npair, stride=ER), :] = acc[:, j * LANES:(j + 1) * LANES]

        @pl.when(idx + 2 < total)
        def _():
            start(w_load(idx + 2, slot))

    def prefetch(_, c):
        for t in range(tiles):
            y2_load(c * tiles + t, t).start()

    def combine(_, c):
        for g in range(NGRP):
            for kind in (OPA, PUP, PDN, PLO, PHI):
                ag(kind, g, c).wait_recv()
        for t in range(tiles):
            y2_load(c * tiles + t, t).wait()
            if c > 0:
                y_store((c - 1) * tiles + t, t).wait()
        for p in range(pc):
            q = c * pc + p
            t, off = p * rows // DTOK, p * rows % DTOK
            rhs = part[:, :, :, q].reshape(cols, dwidth)
            yt[t, off:off + rows, :] = (dot(mixb[q * rows:(q + 1) * rows, :], rhs)
                                        + y2c[t, off:off + rows, :]).astype(BF16)
        for t in range(tiles):
            y_store(c * tiles + t, t).start()

    for c in range(NCHUNK):
        x_load(c).start()
    start(ws_load())
    barrier = pltpu.get_barrier_semaphore()
    for k in range(1, n):
        pl.semaphore_signal(barrier, inc=1, device_id={'seq': lax.rem(me + k, n)}, device_id_type=MESH)
    zs[...] = jnp.zeros_like(zs)
    phi[...] = dot((gain_ref[0] * unit_rows(phi_ref[...], 0)).astype(BF16), perm_ref[...]).astype(BF16)

    def openings(s, _):
        front(s)

        @pl.when(s == 0)
        def _():
            pl.semaphore_wait(barrier, n - 1)

        for k in range(1, n):
            mx_msg(k, s).start()
        return 0

    lax.fori_loop(0, NCHUNK - 1, openings, 0)
    xn_load(0, 0).start()
    xn_load(1, 1).start()
    numerators(0)
    front(NCHUNK - 1)
    for k in range(1, n):
        mx_msg(k, NCHUNK - 1).start()
    stage1(0, 0)
    numerators(1)

    def more(c, _):
        numerators(c)
        stage1(0, c - 1)
        return 0

    lax.fori_loop(2, NCHUNK, more, 0)
    for c in (NCHUNK - 2, NCHUNK - 1):
        xn_store(c).wait()
    start(w_load(0, 0))
    start(w_load(1, 1))
    stage2(0, 0)

    zt[...] = zs[...].T.reshape(zt.shape)

    def z_msg(k):
        dev = lax.rem(me + k, n)
        return rdma(zt.at[dev % 2, dev // 2], zb.at[me], z_s.at[k - 1], z_r.at[k - 1], dev)

    for k in range(1, n):
        z_msg(k).start()

    for cp in ws_load():
        cp.wait()

    def steps(count, one, events):
        def body(i, _):
            one(i)
            for at, what, g, c in events:
                if at < count:
                    @pl.when(i == at)
                    def _():
                        what(g, c)
            return 0

        lax.fori_loop(0, count, body, 0)
        for at, what, g, c in events:
            if at >= count:
                what(g, c)

    def dense_at(_, i):
        dense_tile(i)

    stage1(0, NCHUNK - 1)
    stage2(0, 1)

    steps(DENSE_A, dense_tile, ((0, stage2, 0, 2), (2, stage2, 0, 3), (2, stage1, 1, 0), (3, stage1, 1, 1),
                                (3, stage1, 1, 2), (3, stage1, 1, 3)))
    for k in range(1, n):
        z_msg(k).wait_recv()
    ztot = zt[core, chip]
    for k in range(1, n):
        ztot = ztot + zb[lax.rem(me + n - k, n)]
    zo[...] = ztot
    run3(0)

    total = NGRP * ER
    steps(ER, lambda e: expert(0, e, total),
          ((1, stage2, 1, 0), (1, dense_at, 0, DENSE_A), (3, stage2, 1, 1), (4, stage2, 1, 2),
           (5, dense_at, 0, DENSE_A + 1), (5, stage2, 1, 3)))
    pack(0)
    for c in range(NCHUNK):
        send_own(0, c)
    run3(1)

    steps(ER, lambda e: expert(1, e, total),
          ((1, dense_at, 0, DENSE_A + 2), (1, relay1, 0, 0), (3, relay1, 0, 1), (5, relay1, 0, 2),
           (5, dense_at, 0, DENSE_A + 3), (5, relay1, 0, 3)))
    pack(1)
    send_own(1, 0)
    send_own(1, 1)

    before = DENSE_A + 4
    steps(dtiles - before, lambda i: dense_tile(before + i),
          ((0, relay2, 0, 0), (0, relay2, 0, 1), (0, relay2, 0, 2), (0, relay2, 0, 3), (0, prefetch, 0, 0),
           (1, relay1, 1, 0), (1, send_own, 1, 2),
           (3, relay1, 1, 1), (3, send_own, 1, 3), (4, relay2, 1, 0), (5, relay1, 1, 2), (5, combine, 0, 0),
           (5, prefetch, 0, 1), (6, relay2, 1, 1), (6, combine, 0, 1), (6, prefetch, 0, 2), (6, relay1, 1, 3)))
    for i in (dtiles - 2, dtiles - 1):
        y2_store(i, i % 2).wait()
    relay2(1, 2)
    combine(0, 2)
    prefetch(0, 3)
    relay2(1, 3)
    combine(0, 3)

    for t in range(tiles):
        y_store(dtiles - tiles + t, t).wait()
    for k in range(1, n):
        z_msg(k).wait_send()

    def drain(c, _):
        for k in range(1, n):
            mx_msg(k, c).wait_send()
        for g in range(NGRP):
            for kind in range(9):
                ag(kind, g, c).wait_send()
        return 0

    lax.fori_loop(0, NCHUNK, drain, 0)


def solution(mesh):
    n = mesh.shape['seq']
    chips = n // 2
    tok_spec = P('data', 'seq', None)
    expert_spec = P('seq', None, None)

    def per_device(x_blk, len_blk, phi_slots, scale_g, w_in_blk, w_out_blk, ws_in, ws_out):
        batch, tok, width = x_blk.shape
        slots = phi_slots.shape[1]
        hidden = ws_in.shape[1]
        cols = 2 * slots
        npair = batch // 2
        ntok = batch * tok
        x2 = x_blk.reshape(ntok, width)
        col = np.arange(cols)
        slot = ((col // 16 % chips * 2 + col // (16 * chips) % 2) * NGRP + col // (32 * chips)) * ER + col % ER
        perm = jnp.asarray(np.arange(slots)[:, None] == slot[None, :], BF16)

        pc = npair // NCHUNK
        rows = 2 * tok
        any_spec = pl.BlockSpec(memory_space=pl.ANY)
        sem = pltpu.SemaphoreType.DMA
        y, _, _ = pl.pallas_call(
            functools.partial(mega_kernel, n, tok),
            in_specs=[pl.BlockSpec(memory_space=pltpu.SMEM), pl.BlockSpec(memory_space=pltpu.SMEM),
                      pl.BlockSpec(memory_space=pltpu.VMEM), pl.BlockSpec(memory_space=pltpu.VMEM),
                      any_spec, any_spec, any_spec, any_spec, any_spec],
            out_specs=[any_spec, any_spec, any_spec],
            out_shape=[jax.ShapeDtypeStruct((ntok, width), BF16),
                       jax.ShapeDtypeStruct((ntok, width), F32),
                       jax.ShapeDtypeStruct((ntok, width), BF16)],
            scratch_shapes=[
                pltpu.VMEM((NGRP, 2, chips, npair, 16, width), BF16),
                pltpu.VMEM((NGRP, chips, npair, 16, width), BF16),
                pltpu.VMEM((2, NGRP, npair // 2, 16, width), BF16),
                pltpu.VMEM((2, NGRP, npair, 16, width), BF16),
                pltpu.VMEM((width, hidden), BF16),
                pltpu.VMEM((hidden, width), BF16),
                pltpu.VMEM((2, width, hidden), BF16),
                pltpu.VMEM((2, hidden, width), BF16),
                pltpu.VMEM((ntok, cols), BF16),
                pltpu.VMEM((2, DTOK, width), BF16),
                pltpu.VMEM((2, DTOK, width), F32),
                pltpu.VMEM((pc * rows // DTOK, DTOK, width), F32),
                pltpu.VMEM((pc * rows // DTOK, DTOK, width), BF16),
                pltpu.VMEM((width // LANES, npair * 16, LANES), F32),
                pltpu.VMEM((width, cols), BF16),
                pltpu.VMEM((npair, cols), F32),
                pltpu.VMEM((n, npair, cols), F32),
                pltpu.VMEM((npair, cols), F32),
                pltpu.VMEM((LANES, cols // 2), F32),
                pltpu.VMEM((2, chips, 16, LANES), F32),
                pltpu.VMEM((n, 16, LANES), F32),
                pltpu.VMEM((16, LANES), F32),
                sem((7, NGRP, NCHUNK)), sem((7, NGRP, NCHUNK)),
                sem((9, NGRP, NCHUNK)), sem((9, NGRP, NCHUNK)),
                sem((n - 1, NCHUNK)), sem((n - 1, NCHUNK)), sem((n - 1,)), sem((n - 1,)),
                sem((NCHUNK,)), sem((2,)), sem((2,)), sem((2, 2)), sem((2,)), sem((2,)),
                sem((pc * rows // DTOK,)), sem((pc * rows // DTOK,)), pltpu.SemaphoreType.REGULAR((NGRP,)),
            ],
            compiler_params=pltpu.CompilerParams(collective_id=0, has_side_effects=True,
                                                 vmem_limit_bytes=VMEM_BYTES),
            name='mega',
        )(len_blk, scale_g.reshape(1), phi_slots, perm, x2, ws_in, ws_out, w_in_blk, w_out_blk)
        return y.reshape(batch, tok, width)

    return jax.shard_map(per_device, mesh=mesh, in_specs=(tok_spec, P('data'), P(), P(), expert_spec, expert_spec, P(), P()), out_specs=tok_spec, check_vma=False)
```

```python
import functools

import jax
import jax.numpy as jnp
import numpy as np
from jax import lax
from jax.experimental import pallas as pl
from jax.experimental.pallas import tpu as pltpu
from jax.sharding import PartitionSpec as P

NORM_EPS = 1e-6
NEG_BIG = -1e30
F32 = jnp.float32
BF16 = jnp.bfloat16
MESH = pl.DeviceIdType.MESH
LANES = 128
NGRP = 2
NCHUNK = 4
ER = 8
VMEM_BYTES = 67043328
UNROLL = 4
DTOK = 256
DENSE_A = 5

D2D, TUP, TDN, RUP, RDN, SUP, SDN = range(7)
OUP, ODN, OPA, FUP, FDN, PUP, PDN, PLO, PHI = range(9)


def unit_rows(values, axis_id):
    wide_vals = values.astype(F32)
    return wide_vals / jnp.sqrt(jnp.sum(wide_vals * wide_vals, axis=axis_id, keepdims=True) + NORM_EPS)


def dot(a, b):
    return jnp.dot(a, b, preferred_element_type=F32)


def gelu(v):
    return jax.nn.gelu(v, approximate=True)


def mega_kernel(n, tok, len_ref, gain_ref, phi_ref, perm_ref, x_hbm, wsi_hbm, wso_hbm, w1_hbm, w2_hbm,
                y_ref, y2_hbm, xn_hbm,
                part, dbuf, tbuf, rbuf, wsi, wso, w1b, w2b, mixb, xnb, y2b, y2c,
                phi, pm, mxb, mx, zs, zt, zb, zo,
                rs_s, rs_r, ag_s, ag_r, mx_s, mx_r, z_s, z_r, x_sem, xs_sem, ws_sem, w_sem, xn_sem, y2_sem,
                yc_sem, free_sem):
    me = lax.axis_index('seq')
    chip, core = me // 2, me % 2
    chips = n // 2
    mate = chip * 2 + (1 - core)
    cup, cdn, cop = (chip + 1) % chips, (chip + chips - 1) % chips, (chip + 2) % chips
    up, dn = cup * 2 + core, cdn * 2 + core
    npair, cols = pm.shape
    pc = npair // NCHUNK
    ph = pc // 2
    rows = 2 * tok
    crows = pc * rows
    dwidth = phi.shape[0]
    tiles = crows // DTOK
    ntile = dwidth // LANES
    dtiles = y2_hbm.shape[1] // DTOK
    per = w2b.shape[1] // crows

    def rdma(src, dst, ss, rs, dev):
        return pltpu.make_async_remote_copy(src_ref=src, dst_ref=dst, send_sem=ss, recv_sem=rs,
                                            device_id={'seq': dev}, device_id_type=MESH)

    def w2_rows(block, off, size):
        return block // per, pl.ds(pl.multiple_of((block % per) * crows + off, rows), size)

    def tok_rows(c):
        return pl.ds(pl.multiple_of(c * crows, crows), crows)

    def x_load(c):
        b, sl = w2_rows(c, 0, crows)
        return pltpu.make_async_copy(x_hbm.at[tok_rows(c), :], w2b.at[b, sl, :], x_sem.at[c])

    def xn_store(c):
        b, sl = w2_rows(NCHUNK + c % 2, 0, crows)
        return pltpu.make_async_copy(w2b.at[b, sl, :], xn_hbm.at[tok_rows(c), :], xs_sem.at[c % 2])

    def w_load(e, slot):
        return (pltpu.make_async_copy(w1_hbm.at[e], w1b.at[slot], w_sem.at[0, slot]),
                pltpu.make_async_copy(w2_hbm.at[e], w2b.at[slot], w_sem.at[1, slot]))

    def ws_load():
        return (pltpu.make_async_copy(wsi_hbm, wsi, ws_sem.at[0]),
                pltpu.make_async_copy(wso_hbm, wso, ws_sem.at[1]))

    def tile_rows(i):
        return pl.ds(pl.multiple_of(i * DTOK, DTOK), DTOK)

    def xn_load(i, slot):
        return pltpu.make_async_copy(xn_hbm.at[tile_rows(i), :], xnb.at[slot], xn_sem.at[slot])

    def y2_store(i):
        return pltpu.make_async_copy(y2b, y2_hbm.at[:, tile_rows(i), :], y2_sem)

    def y2_load(i, slot):
        return pltpu.make_async_copy(y2_hbm.at[:, tile_rows(i), :], y2c.at[:, tile_rows(slot), :], yc_sem.at[slot])

    def start(copies):
        for cp in copies:
            cp.start()

    def side_by_side(count, one):
        def body(i, _):
            for u in range(UNROLL):
                one(i * UNROLL + u)
            return 0

        lax.fori_loop(0, count // UNROLL, body, 0)

    def all_of(c):
        return pl.ds(c * pc, pc)

    def lo_of(c):
        return pl.ds(c * pc, ph)

    def hi_of(c):
        return pl.ds(c * pc + ph, ph)

    def tb(g, d):
        return tbuf.at[d] if g == 0 else dbuf.at[0, d]

    def rb(g, d):
        return rbuf.at[d] if g == 0 else dbuf.at[0, 2 + d]

    def rs(kind, g, c):
        ss, rr = rs_s.at[kind, g, c], rs_r.at[kind, g, c]
        mine = part.at[g, core]
        if kind == D2D:
            return rdma(part.at[g, 1 - core, :, all_of(c)], dbuf.at[g, :, all_of(c)], ss, rr, mate)
        if kind == TUP:
            return rdma(mine.at[cop, lo_of(c)], tb(g, 0).at[pl.ds(c * ph, ph)], ss, rr, up)
        if kind == TDN:
            return rdma(mine.at[cop, hi_of(c)], tb(g, 1).at[pl.ds(c * ph, ph)], ss, rr, dn)
        if kind == RUP:
            return rdma(mine.at[cup, hi_of(c)], rb(g, 0).at[hi_of(c)], ss, rr, up)
        if kind == RDN:
            return rdma(mine.at[cdn, lo_of(c)], rb(g, 1).at[lo_of(c)], ss, rr, dn)
        if kind == SUP:
            return rdma(mine.at[cup, lo_of(c)], rb(g, 0).at[lo_of(c)], ss, rr, up)
        return rdma(mine.at[cdn, hi_of(c)], rb(g, 1).at[hi_of(c)], ss, rr, dn)

    def stage1(g, c):
        rs(D2D, g, c).wait_recv()

        def body(i, _):
            q = c * pc + i
            a = part[g, core, :, q].astype(F32) + dbuf[g, :, q].astype(F32)
            part[g, core, :, q] = a.astype(BF16)
            return 0

        lax.fori_loop(0, pc, body, 0)
        for kind in (TUP, TDN, RUP, RDN):
            rs(kind, g, c).start()

    def stage2(g, c):
        for kind, nxt, dst, off, d in ((TUP, SUP, cup, 0, 0), (TDN, SDN, cdn, ph, 1)):
            rs(kind, g, c).wait_recv()

            def body(i, _):
                q = c * pc + off + i
                a = part[g, core, dst, q].astype(F32) + tb(g, d)[c * ph + i].astype(F32)
                part[g, core, dst, q] = a.astype(BF16)
                return 0

            lax.fori_loop(0, ph, body, 0)
            rs(nxt, g, c).start()

    def stage3(g, c):
        for kind in (RUP, RDN, SUP, SDN):
            rs(kind, g, c).wait_recv()
        zg = zo[...]
        lane = lax.broadcasted_iota(jnp.int32, zg.shape, 1)

        def one(i):
            q = c * pc + i
            z = jnp.sum(jnp.where(lane == g * npair + q, zg, 0.0), axis=1, keepdims=True)
            a = part[g, core, chip, q].astype(F32) + rb(g, 0)[q].astype(F32) + rb(g, 1)[q].astype(F32)
            a = a / z
            for j in range(ntile):
                y2c[j, pl.ds(pl.multiple_of(q * 16, 16), 16), :] = a[:, j * LANES:(j + 1) * LANES]

        side_by_side(pc, one)

    def run3(g):
        def body(c, _):
            stage3(g, c)
            return 0

        lax.fori_loop(0, NCHUNK, body, 0)

        def sent(c, _):
            for kind in range(7):
                rs(kind, g, c).wait_send()
            return 0

        lax.fori_loop(0, NCHUNK, sent, 0)
        for dev in (up, dn, mate):
            pl.semaphore_signal(free_sem.at[g], inc=1, device_id={'seq': dev}, device_id_type=MESH)

    def ag(kind, g, c):
        origin, part_of, dev = {OUP: (chip, all_of, up), ODN: (chip, all_of, dn), OPA: (chip, all_of, mate),
                                FUP: (cdn, lo_of, up), FDN: (cup, hi_of, dn),
                                PUP: (cdn, all_of, mate), PDN: (cup, all_of, mate),
                                PLO: (cop, lo_of, mate), PHI: (cop, hi_of, mate)}[kind]
        ref = part.at[g, core, origin, part_of(c)]
        return rdma(ref, ref, ag_s.at[kind, g, c], ag_r.at[kind, g, c], dev)

    def send_own(g, c):
        for kind in (OUP, ODN, OPA):
            ag(kind, g, c).start()

    def pack(g):
        def body(q, _):
            for j in range(ntile):
                part[g, core, chip, q, :, j * LANES:(j + 1) * LANES] = (
                    y2c[j, pl.ds(pl.multiple_of(q * 16, 16), 16), :].astype(BF16))
            return 0

        lax.fori_loop(0, npair, body, 0)
        pl.semaphore_wait(free_sem.at[g], 3)

    def relay1(g, c):
        ag(OUP, g, c).wait_recv()
        ag(FUP, g, c).start()
        ag(PUP, g, c).start()
        ag(ODN, g, c).wait_recv()
        ag(FDN, g, c).start()
        ag(PDN, g, c).start()

    def relay2(g, c):
        ag(FUP, g, c).wait_recv()
        ag(PLO, g, c).start()
        ag(FDN, g, c).wait_recv()
        ag(PHI, g, c).start()

    nblk = cols // LANES

    def logit_at(c, p, j):
        return c % (NCHUNK - 1) * nblk + j, pl.ds(pl.multiple_of(p * rows, rows), rows)

    def front(c):
        x_load(c).wait()

        @pl.when(c >= 2)
        def _():
            xn_store(c - 2).wait()

        first = me * tok

        def one(p):
            q = c * pc + p
            b, sl = w2_rows(c, p * rows, rows)
            x = w2b[b, sl, :].astype(F32)
            inv = lax.rsqrt(jnp.sum(x * x, axis=1, keepdims=True) + NORM_EPS)
            xn = (x * inv).astype(BF16)
            b, sl = w2_rows(NCHUNK + c % 2, p * rows, rows)
            w2b[b, sl, :] = xn
            logits = dot(xn, phi[...])
            ri = lax.broadcasted_iota(jnp.int32, (rows, cols), 0)
            ci = lax.broadcasted_iota(jnp.int32, (rows, cols), 1)
            odd = ri >= tok
            same = jnp.where(odd, 1, 0) == ((ci >> 3) & 1)
            lim = jnp.where(odd, len_ref[2 * q + 1], len_ref[2 * q])
            valid = (first + (ri & (tok - 1))) < lim
            own = jnp.where(same, logits, NEG_BIG)
            top = jnp.max(own, axis=1, keepdims=True)
            ex = jnp.exp(own - top)
            mixb[pl.ds(pl.multiple_of(q * rows, rows), rows), :] = (
                ex * (1.0 / jnp.sum(ex, axis=1, keepdims=True))).astype(BF16)
            lm = jnp.where(valid, own, NEG_BIG)
            for j in range(nblk):
                b, sl = logit_at(c, p, j)
                y2c[b, sl, :] = lm[:, j * LANES:(j + 1) * LANES]
            pm[pl.ds(q, 1), :] = jnp.max(lm, axis=0, keepdims=True)

        side_by_side(pc, one)
        xn_store(c).start()

    def mx_msg(k, c):
        sl = pl.ds(pl.multiple_of(c * pc, pc), pc)
        return rdma(pm.at[sl, :], mxb.at[me, sl, :], mx_s.at[k - 1, c], mx_r.at[k - 1, c], lax.rem(me + k, n))

    half = cols // 2

    def numerators(c):
        sl = pl.ds(pl.multiple_of(c * pc, pc), pc)
        for k in range(1, n):
            mx_msg(k, c).wait_recv()
        top = pm[sl, :]
        for k in range(1, n):
            top = jnp.maximum(top, mxb[lax.rem(me + n - k, n), sl, :])
        mx[sl, :] = top

        def one(p):
            q = c * pc + p
            lm = []
            for j in range(nblk):
                b, sl = logit_at(c, p, j)
                lm.append(y2c[b, sl, :])
            e = jnp.exp(jnp.concatenate(lm, axis=1) - mx[pl.ds(q, 1), :])
            z = jnp.sum(e, axis=0, keepdims=True)
            zs[pl.ds(q, 1), :] = z[:, :half]
            zs[pl.ds(npair + q, 1), :] = z[:, half:]
            b, xsl = w2_rows(c, p * rows, rows)
            num = lax.dot_general(e.astype(BF16), w2b[b, xsl, :], (((0,), (0,)), ((), ())),
                                  preferred_element_type=F32)
            part[:, :, :, q] = num.astype(BF16).reshape(NGRP, 2, chips, 16, dwidth)

        side_by_side(pc, one)
        for g in range(NGRP):
            rs(D2D, g, c).start()

    def dense_tile(i):
        slot = i % 2
        xn_load(i, slot).wait()
        xt = xnb[slot]
        hidden = wsi.shape[1]
        step = min(hidden, 768)
        acc = None
        for f in range(0, hidden, step):
            h = gelu(dot(xt, wsi[:, f:f + step])).astype(BF16)
            o = dot(h, wso[f:f + step, :])
            acc = o if acc is None else acc + o

        @pl.when(i >= 1)
        def _():
            y2_store(i - 1).wait()

        for j in range(ntile):
            y2b[j] = acc[:, j * LANES:(j + 1) * LANES]
        y2_store(i).start()

        @pl.when(i + 2 < dtiles)
        def _():
            xn_load(i + 2, slot).start()

    def expert(g, e, total):
        idx = g * ER + e
        slot = idx % 2
        xin = jnp.concatenate([y2c[j, pl.ds(e, 2 * npair, stride=ER), :] for j in range(ntile)], axis=1).astype(BF16)
        l1, l2 = w_load(idx, slot)
        l1.wait()
        l2.wait()
        hidden = w1b.shape[2]
        step = min(hidden, 768)
        acc = None
        for f in range(0, hidden, step):
            h = gelu(dot(xin, w1b[slot, :, f:f + step])).astype(BF16)
            o = dot(h, w2b[slot, f:f + step, :])
            acc = o if acc is None else acc + o
        for j in range(ntile):
            y2c[j, pl.ds(e, 2 * npair, stride=ER), :] = acc[:, j * LANES:(j + 1) * LANES]

        @pl.when(idx + 2 < total)
        def _():
            start(w_load(idx + 2, slot))

    def prefetch(_, c):
        for t in range(tiles):
            y2_load(c * tiles + t, t).start()

    def combine(_, c):
        for g in range(NGRP):
            for kind in (OPA, PUP, PDN, PLO, PHI):
                ag(kind, g, c).wait_recv()
        for t in range(tiles):
            y2_load(c * tiles + t, t).wait()
        for p in range(pc):
            q = c * pc + p
            rhs = part[:, :, :, q].reshape(cols, dwidth)
            o = dot(mixb[q * rows:(q + 1) * rows, :], rhs)
            for j in range(ntile):
                y_ref[q * rows:(q + 1) * rows, j * LANES:(j + 1) * LANES] = (
                    o[:, j * LANES:(j + 1) * LANES] + y2c[j, p * rows:(p + 1) * rows, :]).astype(BF16)

    for c in range(NCHUNK):
        x_load(c).start()
    start(ws_load())
    barrier = pltpu.get_barrier_semaphore()
    for k in range(1, n):
        pl.semaphore_signal(barrier, inc=1, device_id={'seq': lax.rem(me + k, n)}, device_id_type=MESH)
    zs[...] = jnp.zeros_like(zs)
    phi[...] = dot((gain_ref[0] * unit_rows(phi_ref[...], 0)).astype(BF16), perm_ref[...]).astype(BF16)

    def openings(s, _):
        front(s)

        @pl.when(s == 0)
        def _():
            pl.semaphore_wait(barrier, n - 1)

        for k in range(1, n):
            mx_msg(k, s).start()
        return 0

    lax.fori_loop(0, NCHUNK - 1, openings, 0)
    xn_load(0, 0).start()
    xn_load(1, 1).start()
    numerators(0)
    front(NCHUNK - 1)
    for k in range(1, n):
        mx_msg(k, NCHUNK - 1).start()
    stage1(0, 0)
    numerators(1)

    def more(c, _):
        numerators(c)
        stage1(0, c - 1)
        return 0

    lax.fori_loop(2, NCHUNK, more, 0)
    for c in (NCHUNK - 2, NCHUNK - 1):
        xn_store(c).wait()
    start(w_load(0, 0))
    start(w_load(1, 1))
    stage2(0, 0)

    zt[...] = zs[...].T.reshape(zt.shape)

    def z_msg(k):
        dev = lax.rem(me + k, n)
        return rdma(zt.at[dev % 2, dev // 2], zb.at[me], z_s.at[k - 1], z_r.at[k - 1], dev)

    for k in range(1, n):
        z_msg(k).start()

    for cp in ws_load():
        cp.wait()

    def steps(count, one, events):
        def body(i, _):
            one(i)
            for at, what, g, c in events:
                if at < count:
                    @pl.when(i == at)
                    def _():
                        what(g, c)
            return 0

        lax.fori_loop(0, count, body, 0)
        for at, what, g, c in events:
            if at >= count:
                what(g, c)

    def dense_at(_, i):
        dense_tile(i)

    stage1(0, NCHUNK - 1)
    stage2(0, 1)

    steps(DENSE_A, dense_tile, ((0, stage2, 0, 2), (2, stage2, 0, 3), (2, stage1, 1, 0), (3, stage1, 1, 1),
                                (3, stage1, 1, 2), (3, stage1, 1, 3)))
    for k in range(1, n):
        z_msg(k).wait_recv()
    ztot = zt[core, chip]
    for k in range(1, n):
        ztot = ztot + zb[lax.rem(me + n - k, n)]
    zo[...] = ztot
    run3(0)

    total = NGRP * ER
    steps(ER, lambda e: expert(0, e, total),
          ((1, stage2, 1, 0), (1, dense_at, 0, DENSE_A), (3, stage2, 1, 1), (4, stage2, 1, 2),
           (5, dense_at, 0, DENSE_A + 1), (5, stage2, 1, 3)))
    pack(0)
    for c in range(NCHUNK):
        send_own(0, c)
    run3(1)

    steps(ER, lambda e: expert(1, e, total),
          ((1, dense_at, 0, DENSE_A + 2), (1, relay1, 0, 0), (3, relay1, 0, 1), (5, relay1, 0, 2),
           (5, dense_at, 0, DENSE_A + 3), (5, relay1, 0, 3)))
    pack(1)
    send_own(1, 0)
    send_own(1, 1)

    before = DENSE_A + 4
    steps(dtiles - before, lambda i: dense_tile(before + i),
          ((0, relay2, 0, 0), (0, relay2, 0, 1), (0, relay2, 0, 2), (0, relay2, 0, 3), (0, prefetch, 0, 0),
           (1, relay1, 1, 0), (1, send_own, 1, 2),
           (3, relay1, 1, 1), (3, send_own, 1, 3), (4, relay2, 1, 0), (5, relay1, 1, 2), (5, combine, 0, 0),
           (5, prefetch, 0, 1), (6, relay2, 1, 1), (6, combine, 0, 1), (6, prefetch, 0, 2), (6, relay1, 1, 3)))
    y2_store(dtiles - 1).wait()
    relay2(1, 2)
    combine(0, 2)
    prefetch(0, 3)
    relay2(1, 3)
    combine(0, 3)

    for k in range(1, n):
        z_msg(k).wait_send()

    def drain(c, _):
        for k in range(1, n):
            mx_msg(k, c).wait_send()
        for g in range(NGRP):
            for kind in range(9):
                ag(kind, g, c).wait_send()
        return 0

    lax.fori_loop(0, NCHUNK, drain, 0)


def solution(mesh):
    n = mesh.shape['seq']
    chips = n // 2
    tok_spec = P('data', 'seq', None)
    expert_spec = P('seq', None, None)

    def per_device(x_blk, len_blk, phi_slots, scale_g, w_in_blk, w_out_blk, ws_in, ws_out):
        batch, tok, width = x_blk.shape
        slots = phi_slots.shape[1]
        hidden = ws_in.shape[1]
        cols = 2 * slots
        npair = batch // 2
        ntok = batch * tok
        x2 = x_blk.reshape(ntok, width)
        col = np.arange(cols)
        slot = ((col // 16 % chips * 2 + col // (16 * chips) % 2) * NGRP + col // (32 * chips)) * ER + col % ER
        perm = jnp.asarray(np.arange(slots)[:, None] == slot[None, :], BF16)

        pc = npair // NCHUNK
        rows = 2 * tok
        any_spec = pl.BlockSpec(memory_space=pl.ANY)
        sem = pltpu.SemaphoreType.DMA
        y, _, _ = pl.pallas_call(
            functools.partial(mega_kernel, n, tok),
            in_specs=[pl.BlockSpec(memory_space=pltpu.SMEM), pl.BlockSpec(memory_space=pltpu.SMEM),
                      pl.BlockSpec(memory_space=pltpu.VMEM), pl.BlockSpec(memory_space=pltpu.VMEM),
                      any_spec, any_spec, any_spec, any_spec, any_spec],
            out_specs=[pl.BlockSpec(memory_space=pltpu.VMEM), any_spec, any_spec],
            out_shape=[pltpu.VMEM((ntok, width), BF16),
                       jax.ShapeDtypeStruct((width // LANES, ntok, LANES), F32),
                       jax.ShapeDtypeStruct((ntok, width), BF16)],
            scratch_shapes=[
                pltpu.VMEM((NGRP, 2, chips, npair, 16, width), BF16),
                pltpu.VMEM((NGRP, chips, npair, 16, width), BF16),
                pltpu.VMEM((2, npair // 2, 16, width), BF16),
                pltpu.VMEM((2, npair, 16, width), BF16),
                pltpu.VMEM((width, hidden), BF16),
                pltpu.VMEM((hidden, width), BF16),
                pltpu.VMEM((2, width, hidden), BF16),
                pltpu.VMEM((2, hidden, width), BF16),
                pltpu.VMEM((ntok, cols), BF16),
                pltpu.VMEM((2, DTOK, width), BF16),
                pltpu.VMEM((width // LANES, DTOK, LANES), F32),
                pltpu.VMEM((width // LANES, pc * rows, LANES), F32),
                pltpu.VMEM((width, cols), BF16),
                pltpu.VMEM((npair, cols), F32),
                pltpu.VMEM((n, npair, cols), F32),
                pltpu.VMEM((npair, cols), F32),
                pltpu.VMEM((LANES, cols // 2), F32),
                pltpu.VMEM((2, chips, 16, LANES), F32),
                pltpu.VMEM((n, 16, LANES), F32),
                pltpu.VMEM((16, LANES), F32),
                sem((7, NGRP, NCHUNK)), sem((7, NGRP, NCHUNK)),
                sem((9, NGRP, NCHUNK)), sem((9, NGRP, NCHUNK)),
                sem((n - 1, NCHUNK)), sem((n - 1, NCHUNK)), sem((n - 1,)), sem((n - 1,)),
                sem((NCHUNK,)), sem((2,)), sem((2,)), sem((2, 2)), sem((2,)), sem(()),
                sem((pc * rows // DTOK,)), pltpu.SemaphoreType.REGULAR((NGRP,)),
            ],
            compiler_params=pltpu.CompilerParams(collective_id=0, has_side_effects=True,
                                                 vmem_limit_bytes=VMEM_BYTES - ntok * width * 2),
            name='mega',
        )(len_blk, scale_g.reshape(1), phi_slots, perm, x2, ws_in, ws_out, w_in_blk, w_out_blk)
        return y.reshape(batch, tok, width)

    return jax.shard_map(per_device, mesh=mesh, in_specs=(tok_spec, P('data'), P(), P(), expert_spec, expert_spec, P(), P()), out_specs=tok_spec, check_vma=False)
```

```python
import functools

import jax
import jax.numpy as jnp
import numpy as np
from jax import lax
from jax.experimental import pallas as pl
from jax.experimental.pallas import tpu as pltpu
from jax.sharding import PartitionSpec as P

NORM_EPS = 1e-6
NEG_BIG = -1e30
F32 = jnp.float32
BF16 = jnp.bfloat16
MESH = pl.DeviceIdType.MESH
LANES = 128
NGRP = 2
NCHUNK = 4
ER = 8
VMEM_BYTES = 67043328
UNROLL = 4
DTOK = 256
DENSE_A = 5

D2D, TUP, TDN, RUP, RDN, SUP, SDN = range(7)
OUP, ODN, OPA, FUP, FDN, PUP, PDN, PLO, PHI = range(9)


def unit_rows(values, axis_id):
    wide_vals = values.astype(F32)
    return wide_vals / jnp.sqrt(jnp.sum(wide_vals * wide_vals, axis=axis_id, keepdims=True) + NORM_EPS)


def dot(a, b):
    return jnp.dot(a, b, preferred_element_type=F32)


def gelu(v):
    return jax.nn.gelu(v, approximate=True)


def mega_kernel(n, tok, len_ref, gain_ref, phi_ref, perm_ref, x_hbm, wsi_hbm, wso_hbm, w1_hbm, w2_hbm,
                y_ref, y2_hbm, xn_hbm,
                part, dbuf, tbuf, rbuf, wsi, wso, w1b, w2b, mixb, xnb, y2b, y2c,
                phi, pm, mxb, mx, zs, zt, zb, zo,
                rs_s, rs_r, ag_s, ag_r, mx_s, mx_r, z_s, z_r, x_sem, xs_sem, ws_sem, w_sem, xn_sem, y2_sem,
                yc_sem, free_sem):
    me = lax.axis_index('seq')
    chip, core = me // 2, me % 2
    chips = n // 2
    mate = chip * 2 + (1 - core)
    cup, cdn, cop = (chip + 1) % chips, (chip + chips - 1) % chips, (chip + 2) % chips
    up, dn = cup * 2 + core, cdn * 2 + core
    npair, cols = pm.shape
    pc = npair // NCHUNK
    ph = pc // 2
    rows = 2 * tok
    crows = pc * rows
    dwidth = phi.shape[0]
    tiles = crows // DTOK
    ntile = dwidth // LANES
    dtiles = y2_hbm.shape[1] // DTOK
    per = w2b.shape[1] // crows

    def rdma(src, dst, ss, rs, dev):
        return pltpu.make_async_remote_copy(src_ref=src, dst_ref=dst, send_sem=ss, recv_sem=rs,
                                            device_id={'seq': dev}, device_id_type=MESH)

    def w2_rows(block, off, size):
        return block // per, pl.ds(pl.multiple_of((block % per) * crows + off, rows), size)

    def tok_rows(c):
        return pl.ds(pl.multiple_of(c * crows, crows), crows)

    def x_load(c):
        b, sl = w2_rows(c, 0, crows)
        return pltpu.make_async_copy(x_hbm.at[tok_rows(c), :], w2b.at[b, sl, :], x_sem.at[c])

    def xn_store(c):
        b, sl = w2_rows(NCHUNK + c % 2, 0, crows)
        return pltpu.make_async_copy(w2b.at[b, sl, :], xn_hbm.at[tok_rows(c), :], xs_sem.at[c % 2])

    def w_load(e, slot):
        return (pltpu.make_async_copy(w1_hbm.at[e], w1b.at[slot], w_sem.at[0, slot]),
                pltpu.make_async_copy(w2_hbm.at[e], w2b.at[slot], w_sem.at[1, slot]))

    def ws_load():
        return (pltpu.make_async_copy(wsi_hbm, wsi, ws_sem.at[0]),
                pltpu.make_async_copy(wso_hbm, wso, ws_sem.at[1]))

    def tile_rows(i):
        return pl.ds(pl.multiple_of(i * DTOK, DTOK), DTOK)

    def xn_load(i, slot):
        return pltpu.make_async_copy(xn_hbm.at[tile_rows(i), :], xnb.at[slot], xn_sem.at[slot])

    def y2_store(i):
        return pltpu.make_async_copy(y2b, y2_hbm.at[:, tile_rows(i), :], y2_sem)

    def y2_load(i, slot):
        return pltpu.make_async_copy(y2_hbm.at[:, tile_rows(i), :], y2c.at[:, tile_rows(slot), :], yc_sem.at[slot])

    def start(copies):
        for cp in copies:
            cp.start()

    def side_by_side(count, one):
        def body(i, _):
            for u in range(UNROLL):
                one(i * UNROLL + u)
            return 0

        lax.fori_loop(0, count // UNROLL, body, 0)

    def all_of(c):
        return pl.ds(c * pc, pc)

    def lo_of(c):
        return pl.ds(c * pc, ph)

    def hi_of(c):
        return pl.ds(c * pc + ph, ph)

    def tb(g, d):
        return tbuf.at[d] if g == 0 else dbuf.at[0, d]

    def rb(g, d):
        return rbuf.at[d] if g == 0 else dbuf.at[0, 2 + d]

    def rs(kind, g, c):
        ss, rr = rs_s.at[kind, g, c], rs_r.at[kind, g, c]
        mine = part.at[g, core]
        if kind == D2D:
            return rdma(part.at[g, 1 - core, :, all_of(c)], dbuf.at[g, :, all_of(c)], ss, rr, mate)
        if kind == TUP:
            return rdma(mine.at[cop, lo_of(c)], tb(g, 0).at[pl.ds(c * ph, ph)], ss, rr, up)
        if kind == TDN:
            return rdma(mine.at[cop, hi_of(c)], tb(g, 1).at[pl.ds(c * ph, ph)], ss, rr, dn)
        if kind == RUP:
            return rdma(mine.at[cup, hi_of(c)], rb(g, 0).at[hi_of(c)], ss, rr, up)
        if kind == RDN:
            return rdma(mine.at[cdn, lo_of(c)], rb(g, 1).at[lo_of(c)], ss, rr, dn)
        if kind == SUP:
            return rdma(mine.at[cup, lo_of(c)], rb(g, 0).at[lo_of(c)], ss, rr, up)
        return rdma(mine.at[cdn, hi_of(c)], rb(g, 1).at[hi_of(c)], ss, rr, dn)

    def stage1(g, c):
        rs(D2D, g, c).wait_recv()

        def body(i, _):
            q = c * pc + i
            a = part[g, core, :, q].astype(F32) + dbuf[g, :, q].astype(F32)
            part[g, core, :, q] = a.astype(BF16)
            return 0

        lax.fori_loop(0, pc, body, 0)
        for kind in (TUP, TDN, RUP, RDN):
            rs(kind, g, c).start()

    def stage2(g, c):
        for kind, nxt, dst, off, d in ((TUP, SUP, cup, 0, 0), (TDN, SDN, cdn, ph, 1)):
            rs(kind, g, c).wait_recv()

            def body(i, _):
                q = c * pc + off + i
                a = part[g, core, dst, q].astype(F32) + tb(g, d)[c * ph + i].astype(F32)
                part[g, core, dst, q] = a.astype(BF16)
                return 0

            lax.fori_loop(0, ph, body, 0)
            rs(nxt, g, c).start()

    def stage3(g, c):
        for kind in (RUP, RDN, SUP, SDN):
            rs(kind, g, c).wait_recv()
        zg = zo[...]
        lane = lax.broadcasted_iota(jnp.int32, zg.shape, 1)

        def one(i):
            q = c * pc + i
            z = jnp.sum(jnp.where(lane == g * npair + q, zg, 0.0), axis=1, keepdims=True)
            a = part[g, core, chip, q].astype(F32) + rb(g, 0)[q].astype(F32) + rb(g, 1)[q].astype(F32)
            a = a / z
            for j in range(ntile):
                y2c[j, pl.ds(pl.multiple_of(q * 16, 16), 16), :] = a[:, j * LANES:(j + 1) * LANES]

        side_by_side(pc, one)

    def run3(g):
        def body(c, _):
            stage3(g, c)
            return 0

        lax.fori_loop(0, NCHUNK, body, 0)

        def sent(c, _):
            for kind in range(7):
                rs(kind, g, c).wait_send()
            return 0

        lax.fori_loop(0, NCHUNK, sent, 0)
        for dev in (up, dn, mate):
            pl.semaphore_signal(free_sem.at[g], inc=1, device_id={'seq': dev}, device_id_type=MESH)

    def ag(kind, g, c):
        origin, part_of, dev = {OUP: (chip, all_of, up), ODN: (chip, all_of, dn), OPA: (chip, all_of, mate),
                                FUP: (cdn, lo_of, up), FDN: (cup, hi_of, dn),
                                PUP: (cdn, all_of, mate), PDN: (cup, all_of, mate),
                                PLO: (cop, lo_of, mate), PHI: (cop, hi_of, mate)}[kind]
        ref = part.at[g, core, origin, part_of(c)]
        return rdma(ref, ref, ag_s.at[kind, g, c], ag_r.at[kind, g, c], dev)

    def send_own(g, c):
        for kind in (OUP, ODN, OPA):
            ag(kind, g, c).start()

    def pack(g):
        def body(q, _):
            for j in range(ntile):
                part[g, core, chip, q, :, j * LANES:(j + 1) * LANES] = (
                    y2c[j, pl.ds(pl.multiple_of(q * 16, 16), 16), :].astype(BF16))
            return 0

        lax.fori_loop(0, npair, body, 0)
        pl.semaphore_wait(free_sem.at[g], 3)

    def relay1(g, c):
        ag(OUP, g, c).wait_recv()
        ag(FUP, g, c).start()
        ag(PUP, g, c).start()
        ag(ODN, g, c).wait_recv()
        ag(FDN, g, c).start()
        ag(PDN, g, c).start()

    def relay2(g, c):
        ag(FUP, g, c).wait_recv()
        ag(PLO, g, c).start()
        ag(FDN, g, c).wait_recv()
        ag(PHI, g, c).start()

    nblk = cols // LANES

    def logit_at(c, p, j):
        return c % (NCHUNK - 1) * nblk + j, pl.ds(pl.multiple_of(p * rows, rows), rows)

    def front(c):
        x_load(c).wait()

        @pl.when(c >= 2)
        def _():
            xn_store(c - 2).wait()

        first = me * tok

        def one(p):
            q = c * pc + p
            b, sl = w2_rows(c, p * rows, rows)
            x = w2b[b, sl, :].astype(F32)
            inv = lax.rsqrt(jnp.sum(x * x, axis=1, keepdims=True) + NORM_EPS)
            xn = (x * inv).astype(BF16)
            b, sl = w2_rows(NCHUNK + c % 2, p * rows, rows)
            w2b[b, sl, :] = xn
            logits = dot(xn, phi[...])
            ri = lax.broadcasted_iota(jnp.int32, (rows, cols), 0)
            ci = lax.broadcasted_iota(jnp.int32, (rows, cols), 1)
            odd = ri >= tok
            same = jnp.where(odd, 1, 0) == ((ci >> 3) & 1)
            lim = jnp.where(odd, len_ref[2 * q + 1], len_ref[2 * q])
            valid = (first + (ri & (tok - 1))) < lim
            own = jnp.where(same, logits, NEG_BIG)
            top = jnp.max(own, axis=1, keepdims=True)
            ex = jnp.exp(own - top)
            mixb[pl.ds(pl.multiple_of(q * rows, rows), rows), :] = (
                ex * (1.0 / jnp.sum(ex, axis=1, keepdims=True))).astype(BF16)
            lm = jnp.where(valid, own, NEG_BIG)
            for j in range(nblk):
                b, sl = logit_at(c, p, j)
                y2c[b, sl, :] = lm[:, j * LANES:(j + 1) * LANES]
            pm[pl.ds(q, 1), :] = jnp.max(lm, axis=0, keepdims=True)

        side_by_side(pc, one)
        xn_store(c).start()

    def mx_msg(k, c):
        sl = pl.ds(pl.multiple_of(c * pc, pc), pc)
        return rdma(pm.at[sl, :], mxb.at[me, sl, :], mx_s.at[k - 1, c], mx_r.at[k - 1, c], lax.rem(me + k, n))

    half = cols // 2

    def numerators(c):
        sl = pl.ds(pl.multiple_of(c * pc, pc), pc)
        for k in range(1, n):
            mx_msg(k, c).wait_recv()
        top = pm[sl, :]
        for k in range(1, n):
            top = jnp.maximum(top, mxb[lax.rem(me + n - k, n), sl, :])
        mx[sl, :] = top

        def one(p):
            q = c * pc + p
            lm = []
            for j in range(nblk):
                b, sl = logit_at(c, p, j)
                lm.append(y2c[b, sl, :])
            e = jnp.exp(jnp.concatenate(lm, axis=1) - mx[pl.ds(q, 1), :])
            z = jnp.sum(e, axis=0, keepdims=True)
            zs[pl.ds(q, 1), :] = z[:, :half]
            zs[pl.ds(npair + q, 1), :] = z[:, half:]
            b, xsl = w2_rows(c, p * rows, rows)
            num = lax.dot_general(e.astype(BF16), w2b[b, xsl, :], (((0,), (0,)), ((), ())),
                                  preferred_element_type=F32)
            part[:, :, :, q] = num.astype(BF16).reshape(NGRP, 2, chips, 16, dwidth)

        side_by_side(pc, one)
        for g in range(NGRP):
            rs(D2D, g, c).start()

    def dense_tile(i):
        slot = i % 2
        xn_load(i, slot).wait()
        xt = xnb[slot]
        hidden = wsi.shape[1]
        step = min(hidden, 768)
        acc = None
        for f in range(0, hidden, step):
            h = gelu(dot(xt, wsi[:, f:f + step])).astype(BF16)
            o = dot(h, wso[f:f + step, :])
            acc = o if acc is None else acc + o

        @pl.when(i >= 1)
        def _():
            y2_store(i - 1).wait()

        for j in range(ntile):
            y2b[j] = acc[:, j * LANES:(j + 1) * LANES]
        y2_store(i).start()

        @pl.when(i + 2 < dtiles)
        def _():
            xn_load(i + 2, slot).start()

    def expert(g, e, total):
        idx = g * ER + e
        slot = idx % 2
        xin = jnp.concatenate([y2c[j, pl.ds(e, 2 * npair, stride=ER), :] for j in range(ntile)], axis=1).astype(BF16)
        l1, l2 = w_load(idx, slot)
        l1.wait()
        l2.wait()
        acc = dot(gelu(dot(xin, w1b[slot])).astype(BF16), w2b[slot])
        for j in range(ntile):
            y2c[j, pl.ds(e, 2 * npair, stride=ER), :] = acc[:, j * LANES:(j + 1) * LANES]

        @pl.when(idx + 2 < total)
        def _():
            start(w_load(idx + 2, slot))

    def prefetch(_, c):
        for t in range(tiles):
            y2_load(c * tiles + t, t).start()

    def combine(_, c):
        for g in range(NGRP):
            for kind in (OPA, PUP, PDN, PLO, PHI):
                ag(kind, g, c).wait_recv()
        for t in range(tiles):
            y2_load(c * tiles + t, t).wait()
        for p in range(pc):
            q = c * pc + p
            rhs = part[:, :, :, q].reshape(cols, dwidth)
            o = dot(mixb[q * rows:(q + 1) * rows, :], rhs)
            for j in range(ntile):
                y_ref[q * rows:(q + 1) * rows, j * LANES:(j + 1) * LANES] = (
                    o[:, j * LANES:(j + 1) * LANES] + y2c[j, p * rows:(p + 1) * rows, :]).astype(BF16)

    for c in range(NCHUNK):
        x_load(c).start()
    start(ws_load())
    barrier = pltpu.get_barrier_semaphore()
    for k in range(1, n):
        pl.semaphore_signal(barrier, inc=1, device_id={'seq': lax.rem(me + k, n)}, device_id_type=MESH)
    zs[...] = jnp.zeros_like(zs)
    phi[...] = dot((gain_ref[0] * unit_rows(phi_ref[...], 0)).astype(BF16), perm_ref[...]).astype(BF16)

    def openings(s, _):
        front(s)

        @pl.when(s == 0)
        def _():
            pl.semaphore_wait(barrier, n - 1)

        for k in range(1, n):
            mx_msg(k, s).start()
        return 0

    lax.fori_loop(0, NCHUNK - 1, openings, 0)
    xn_load(0, 0).start()
    xn_load(1, 1).start()
    numerators(0)
    front(NCHUNK - 1)
    for k in range(1, n):
        mx_msg(k, NCHUNK - 1).start()
    stage1(0, 0)
    numerators(1)

    def more(c, _):
        numerators(c)
        stage1(0, c - 1)
        return 0

    lax.fori_loop(2, NCHUNK, more, 0)
    for c in (NCHUNK - 2, NCHUNK - 1):
        xn_store(c).wait()
    start(w_load(0, 0))
    start(w_load(1, 1))
    stage2(0, 0)

    zt[...] = zs[...].T.reshape(zt.shape)

    def z_msg(k):
        dev = lax.rem(me + k, n)
        return rdma(zt.at[dev % 2, dev // 2], zb.at[me], z_s.at[k - 1], z_r.at[k - 1], dev)

    for k in range(1, n):
        z_msg(k).start()

    for cp in ws_load():
        cp.wait()

    def steps(count, one, events):
        def body(i, _):
            one(i)
            for at, what, g, c in events:
                if at < count:
                    @pl.when(i == at)
                    def _():
                        what(g, c)
            return 0

        lax.fori_loop(0, count, body, 0)
        for at, what, g, c in events:
            if at >= count:
                what(g, c)

    def dense_at(_, i):
        dense_tile(i)

    stage1(0, NCHUNK - 1)
    stage2(0, 1)

    steps(DENSE_A, dense_tile, ((0, stage2, 0, 2), (2, stage2, 0, 3), (2, stage1, 1, 0), (3, stage1, 1, 1),
                                (3, stage1, 1, 2), (3, stage1, 1, 3)))
    for k in range(1, n):
        z_msg(k).wait_recv()
    ztot = zt[core, chip]
    for k in range(1, n):
        ztot = ztot + zb[lax.rem(me + n - k, n)]
    zo[...] = ztot
    run3(0)

    total = NGRP * ER
    steps(ER, lambda e: expert(0, e, total),
          ((1, stage2, 1, 0), (1, dense_at, 0, DENSE_A), (3, stage2, 1, 1), (4, stage2, 1, 2),
           (5, dense_at, 0, DENSE_A + 1), (5, stage2, 1, 3)))
    pack(0)
    for c in range(NCHUNK):
        send_own(0, c)
    run3(1)

    steps(ER, lambda e: expert(1, e, total),
          ((1, dense_at, 0, DENSE_A + 2), (1, relay1, 0, 0), (3, relay1, 0, 1), (5, relay1, 0, 2),
           (5, dense_at, 0, DENSE_A + 3), (5, relay1, 0, 3)))
    pack(1)
    send_own(1, 0)
    send_own(1, 1)

    before = DENSE_A + 4
    steps(dtiles - before, lambda i: dense_tile(before + i),
          ((0, relay2, 0, 0), (0, relay2, 0, 1), (0, relay2, 0, 2), (0, relay2, 0, 3), (0, prefetch, 0, 0),
           (1, relay1, 1, 0), (1, send_own, 1, 2),
           (3, relay1, 1, 1), (3, send_own, 1, 3), (4, relay2, 1, 0), (5, relay1, 1, 2), (5, combine, 0, 0),
           (5, prefetch, 0, 1), (6, relay2, 1, 1), (6, combine, 0, 1), (6, prefetch, 0, 2), (6, relay1, 1, 3)))
    y2_store(dtiles - 1).wait()
    relay2(1, 2)
    combine(0, 2)
    prefetch(0, 3)
    relay2(1, 3)
    combine(0, 3)

    for k in range(1, n):
        z_msg(k).wait_send()

    def drain(c, _):
        for k in range(1, n):
            mx_msg(k, c).wait_send()
        for g in range(NGRP):
            for kind in range(9):
                ag(kind, g, c).wait_send()
        return 0

    lax.fori_loop(0, NCHUNK, drain, 0)


def solution(mesh):
    n = mesh.shape['seq']
    chips = n // 2
    tok_spec = P('data', 'seq', None)
    expert_spec = P('seq', None, None)

    def per_device(x_blk, len_blk, phi_slots, scale_g, w_in_blk, w_out_blk, ws_in, ws_out):
        batch, tok, width = x_blk.shape
        slots = phi_slots.shape[1]
        hidden = ws_in.shape[1]
        cols = 2 * slots
        npair = batch // 2
        ntok = batch * tok
        x2 = x_blk.reshape(ntok, width)
        col = np.arange(cols)
        slot = ((col // 16 % chips * 2 + col // (16 * chips) % 2) * NGRP + col // (32 * chips)) * ER + col % ER
        perm = jnp.asarray(np.arange(slots)[:, None] == slot[None, :], BF16)

        pc = npair // NCHUNK
        rows = 2 * tok
        any_spec = pl.BlockSpec(memory_space=pl.ANY)
        sem = pltpu.SemaphoreType.DMA
        y, _, _ = pl.pallas_call(
            functools.partial(mega_kernel, n, tok),
            in_specs=[pl.BlockSpec(memory_space=pltpu.SMEM), pl.BlockSpec(memory_space=pltpu.SMEM),
                      pl.BlockSpec(memory_space=pltpu.VMEM), pl.BlockSpec(memory_space=pltpu.VMEM),
                      any_spec, any_spec, any_spec, any_spec, any_spec],
            out_specs=[pl.BlockSpec(memory_space=pltpu.VMEM), any_spec, any_spec],
            out_shape=[pltpu.VMEM((ntok, width), BF16),
                       jax.ShapeDtypeStruct((width // LANES, ntok, LANES), F32),
                       jax.ShapeDtypeStruct((ntok, width), BF16)],
            scratch_shapes=[
                pltpu.VMEM((NGRP, 2, chips, npair, 16, width), BF16),
                pltpu.VMEM((NGRP, chips, npair, 16, width), BF16),
                pltpu.VMEM((2, npair // 2, 16, width), BF16),
                pltpu.VMEM((2, npair, 16, width), BF16),
                pltpu.VMEM((width, hidden), BF16),
                pltpu.VMEM((hidden, width), BF16),
                pltpu.VMEM((2, width, hidden), BF16),
                pltpu.VMEM((2, hidden, width), BF16),
                pltpu.VMEM((ntok, cols), BF16),
                pltpu.VMEM((2, DTOK, width), BF16),
                pltpu.VMEM((width // LANES, DTOK, LANES), F32),
                pltpu.VMEM((width // LANES, pc * rows, LANES), F32),
                pltpu.VMEM((width, cols), BF16),
                pltpu.VMEM((npair, cols), F32),
                pltpu.VMEM((n, npair, cols), F32),
                pltpu.VMEM((npair, cols), F32),
                pltpu.VMEM((LANES, cols // 2), F32),
                pltpu.VMEM((2, chips, 16, LANES), F32),
                pltpu.VMEM((n, 16, LANES), F32),
                pltpu.VMEM((16, LANES), F32),
                sem((7, NGRP, NCHUNK)), sem((7, NGRP, NCHUNK)),
                sem((9, NGRP, NCHUNK)), sem((9, NGRP, NCHUNK)),
                sem((n - 1, NCHUNK)), sem((n - 1, NCHUNK)), sem((n - 1,)), sem((n - 1,)),
                sem((NCHUNK,)), sem((2,)), sem((2,)), sem((2, 2)), sem((2,)), sem(()),
                sem((pc * rows // DTOK,)), pltpu.SemaphoreType.REGULAR((NGRP,)),
            ],
            compiler_params=pltpu.CompilerParams(collective_id=0, has_side_effects=True,
                                                 vmem_limit_bytes=VMEM_BYTES - ntok * width * 2),
            name='mega',
        )(len_blk, scale_g.reshape(1), phi_slots, perm, x2, ws_in, ws_out, w_in_blk, w_out_blk)
        return y.reshape(batch, tok, width)

    return jax.shard_map(per_device, mesh=mesh, in_specs=(tok_spec, P('data'), P(), P(), expert_spec, expert_spec, P(), P()), out_specs=tok_spec, check_vma=False)
```
